128 devices in a mesh: cp: 4 (over x), fsdp: 32 (over z, y, core).
Axes of the slice: x: 4, y: 4, z: 4, core: 2. Of those that a mesh axis runs over, the one named last changes fastest.
Arguments:
- tokens: int32 [64, 1024], P('fsdp', 'cp')
- lengths: int32 [64], P('fsdp')
- embed_table: bfloat16 [33, 1280], replicated
- layer_vecs: float32 [9, 1280], P(None, 'fsdp')
- w_qkv: bfloat16 [1280, 3, 20, 64], P('fsdp')
- w_out: bfloat16 [1280, 1280], P('fsdp')
- w_up: bfloat16 [1280, 5120], P('fsdp')
- b_up: float32 [5120], P('fsdp')
- w_down: bfloat16 [5120, 1280], P('fsdp')
- grad_out: bfloat16 [64, 1024, 1280], P('fsdp', 'cp')
Outputs:
- output 1: bfloat16 [64, 1024, 1280], P('fsdp', 'cp')
- output 2: float32 [33, 1280], replicated
- output 3: float32 [9, 1280], P(None, 'fsdp')
- output 4: float32 [1280, 3, 20, 64], P('fsdp')
- output 5: float32 [1280, 1280], P('fsdp')
- output 6: float32 [1280, 5120], P('fsdp')
- output 7: float32 [5120], P('fsdp')
- output 8: float32 [5120, 1280], P('fsdp')
All inputs are finite; a program needn't handle non-finite values.
Results may differ from the reference program's by a relative error of at most 0.00862362.
Values are sent between devices in bfloat16 or wider.
A program may use at most 1 GiB of HBM per device.

```python
import jax
import jax.numpy as jnp
from jax import lax

NUM_SEQS = 64
SEQ_LEN = 1024
MODEL_DIM = 1280
NUM_HEADS = 20
FFN_DIM = 5120
VOCAB_SIZE = 33
BOS_ID = 0
PAD_ID = 1
EOS_ID = 2
MASK_ID = 32
HEAD_DIM = MODEL_DIM // NUM_HEADS
LN_EPS = 1e-5
ROPE_BASE = 10000.0
TRAIN_RATIO = 0.15 * 0.8
NEG_BIG = -1e30


def draw_tokens(rng_key):
    key_list = jax.random.split(rng_key, 4)
    lengths = jax.random.randint(key_list[0], (NUM_SEQS,), SEQ_LEN // 4, SEQ_LEN + 1)
    lengths = lengths.at[0].set(SEQ_LEN).at[1].set(SEQ_LEN // 4)
    positions = jnp.arange(SEQ_LEN)[None, :]
    len_col = lengths[:, None]
    residues = jax.random.randint(key_list[1], (NUM_SEQS, SEQ_LEN), 4, 31)
    win_start = jax.random.randint(key_list[2], (NUM_SEQS, 1), 0, SEQ_LEN)
    in_win = (positions >= win_start) & (positions < win_start + SEQ_LEN // 4)
    hit_draw = jax.random.randint(key_list[3], (NUM_SEQS, SEQ_LEN), 0, 100)
    is_mask = hit_draw < jnp.where(in_win, 45, 5)
    tokens = jnp.where(is_mask, MASK_ID, residues)
    tokens = jnp.where(positions >= len_col, PAD_ID, tokens)
    tokens = jnp.where(positions == len_col - 1, EOS_ID, tokens)
    tokens = jnp.where(positions == 0, BOS_ID, tokens)
    return tokens.astype(jnp.int32), lengths.astype(jnp.int32)


def setup_inputs(seed: int = 0) -> dict:
    key_list = jax.random.split(jax.random.key(seed), 9)
    tokens, lengths = draw_tokens(key_list[0])
    embed_table = jax.random.normal(key_list[1], (VOCAB_SIZE, MODEL_DIM), jnp.float32)
    row_scale = jnp.array([0.2, 0.3, 0.3, 0.3, SEQ_LEN ** -0.5, 0.3, 0.2, 0.3, 0.3], jnp.float32)
    row_shift = jnp.array([1.0, 0.0, 0.0, 0.0, 0.0, 0.0, 1.0, 0.0, 0.0], jnp.float32)
    layer_vecs = row_shift[:, None] + row_scale[:, None] * jax.random.normal(key_list[2], (9, MODEL_DIM), jnp.float32)
    w_qkv = jax.random.normal(key_list[3], (MODEL_DIM, 3, NUM_HEADS, HEAD_DIM), jnp.float32) * MODEL_DIM ** -0.5
    w_out = jax.random.normal(key_list[4], (MODEL_DIM, MODEL_DIM), jnp.float32) * (SEQ_LEN / (2.0 * MODEL_DIM)) ** 0.5
    w_up = jax.random.normal(key_list[5], (MODEL_DIM, FFN_DIM), jnp.float32) * MODEL_DIM ** -0.5
    b_up = 0.5 * jax.random.normal(key_list[6], (FFN_DIM,), jnp.float32)
    w_down = jax.random.normal(key_list[7], (FFN_DIM, MODEL_DIM), jnp.float32) * FFN_DIM ** -0.5
    grad_out = jax.random.normal(key_list[8], (NUM_SEQS, SEQ_LEN, MODEL_DIM), jnp.float32)
    return {
        'tokens': tokens,
        'lengths': lengths,
        'embed_table': embed_table.astype(jnp.bfloat16),
        'layer_vecs': layer_vecs,
        'w_qkv': w_qkv.astype(jnp.bfloat16),
        'w_out': w_out.astype(jnp.bfloat16),
        'w_up': w_up.astype(jnp.bfloat16),
        'b_up': b_up,
        'w_down': w_down.astype(jnp.bfloat16),
        'grad_out': grad_out.astype(jnp.bfloat16),
    }


def rounded(z_in):
    return z_in + lax.stop_gradient(z_in.astype(jnp.bfloat16).astype(jnp.float32) - z_in)


def layer_norm(z_in, ln_gain, ln_bias):
    row_mean = jnp.mean(z_in, axis=-1, keepdims=True)
    centered = z_in - row_mean
    row_var = jnp.mean(centered * centered, axis=-1, keepdims=True)
    return centered * lax.rsqrt(row_var + LN_EPS) * ln_gain + ln_bias


def rotate(z_in, cos_t, sin_t):
    lower_half, upper_half = jnp.split(z_in, 2, axis=-1)
    return jnp.concatenate([lower_half * cos_t - upper_half * sin_t, upper_half * cos_t + lower_half * sin_t], axis=-1)


def one_sequence(params, embed_f32, tok_row, len_row):
    layer_vecs, w_qkv, w_out, w_up, b_up, w_down = params
    positions = jnp.arange(SEQ_LEN)
    is_mask = tok_row == MASK_ID
    key_valid = positions < len_row
    n_mask = jnp.sum(is_mask.astype(jnp.float32))
    drop_scale = (1.0 - TRAIN_RATIO) / (1.0 - n_mask / len_row.astype(jnp.float32))
    keep_scale = jnp.where(is_mask | jnp.logical_not(key_valid), 0.0, drop_scale)
    embedded = embed_f32[tok_row] * keep_scale[:, None]
    norm_in = rounded(layer_norm(embedded, layer_vecs[0], layer_vecs[1]))
    qkv_lin = jnp.dot(norm_in, w_qkv.reshape(MODEL_DIM, 3 * MODEL_DIM)) + layer_vecs[2:5].reshape(3 * MODEL_DIM)
    qkv_lin = qkv_lin.reshape(SEQ_LEN, 3, NUM_HEADS, HEAD_DIM)
    inv_freq = 1.0 / (ROPE_BASE ** (jnp.arange(0, HEAD_DIM, 2, dtype=jnp.float32) / HEAD_DIM))
    angles = positions.astype(jnp.float32)[:, None] * inv_freq[None, :]
    cos_t = jnp.cos(angles)[:, None, :]
    sin_t = jnp.sin(angles)[:, None, :]
    q_heads = rounded(rotate(qkv_lin[:, 0] * HEAD_DIM ** -0.5, cos_t, sin_t))
    k_heads = rounded(rotate(qkv_lin[:, 1], cos_t, sin_t))
    v_heads = rounded(qkv_lin[:, 2])

    def one_head(head_in):
        q_h, k_h, v_h = head_in
        scores = jnp.dot(q_h, k_h.T)
        scores = jnp.where(key_valid[None, :], scores, NEG_BIG)
        return jnp.dot(jax.nn.softmax(scores, axis=-1), v_h)

    per_head = lax.map(jax.checkpoint(one_head), (q_heads.transpose(1, 0, 2), k_heads.transpose(1, 0, 2), v_heads.transpose(1, 0, 2)))
    attn_out = rounded(per_head.transpose(1, 0, 2).reshape(SEQ_LEN, MODEL_DIM))
    resid_mid = embedded + jnp.dot(attn_out, w_out) + layer_vecs[5]
    norm_mid = rounded(layer_norm(resid_mid, layer_vecs[6], layer_vecs[7]))
    gelu_out = rounded(jax.nn.gelu(jnp.dot(norm_mid, w_up) + b_up, approximate=False))
    return resid_mid + jnp.dot(gelu_out, w_down) + layer_vecs[8]


def reference(tokens, lengths, embed_table, layer_vecs, w_qkv, w_out, w_up, b_up, w_down, grad_out):
    params = (layer_vecs, w_qkv.astype(jnp.float32), w_out.astype(jnp.float32), w_up.astype(jnp.float32), b_up, w_down.astype(jnp.float32))
    seq_fn = jax.checkpoint(one_sequence)

    def forward(params_in, embed_f32):
        def per_row(seq_row):
            return seq_fn(params_in, embed_f32, seq_row[0], seq_row[1])
        return lax.map(per_row, (tokens, lengths))

    layer_out, pullback = jax.vjp(forward, params, embed_table.astype(jnp.float32))
    d_params, d_embed = pullback(grad_out.astype(jnp.float32))
    return (layer_out.astype(jnp.bfloat16), d_embed, d_params[0], d_params[1], d_params[2], d_params[3], d_params[4], d_params[5])
```

```python
import functools

import jax
import jax.numpy as jnp
from jax import lax
from jax.experimental import pallas as pl
from jax.experimental.pallas import tpu as pltpu
from jax.sharding import Mesh, PartitionSpec as P

MASK_ID = 32
VOCAB = 33
LN_EPS = 1e-5
ROPE_BASE = 10000.0
TRAIN_RATIO = 0.15 * 0.8
NEG_BIG = -1e30
SEQ = 1024
QLEN = 256
HEADS = 20
HDIM = 64
PAIRS = HEADS // 2
DIM = HEADS * HDIM
ROWS = 40
F32 = jnp.float32
BF16 = jnp.bfloat16
SWAP = [(0, 1), (1, 0)]
CHIP = ('z', 'y')
FSDP = ('z', 'y', 'c')
PADW = 64
HIGH = lax.Precision.HIGHEST


def mm(a, b, dims=((1,), (0,))):
    return lax.dot_general(a, b, (dims, ((), ())), preferred_element_type=F32)


def ln_stats(z_in):
    row_mean = jnp.mean(z_in, axis=-1, keepdims=True)
    centered = z_in - row_mean
    row_var = jnp.mean(centered * centered, axis=-1, keepdims=True)
    inv = lax.rsqrt(row_var + LN_EPS)
    return centered * inv, inv


def ln_back(d_out, gain, xhat, inv):
    d_hat = d_out * gain
    m1 = jnp.mean(d_hat, axis=-1, keepdims=True)
    m2 = jnp.mean(d_hat * xhat, axis=-1, keepdims=True)
    return inv * (d_hat - m1 - xhat * m2)


def expand_qkv(ohk_ref, ohq_ref, tab_ref, csk_ref, csq_ref):
    ohk = ohk_ref[0]
    z_q = mm(ohq_ref[0], tab_ref[0, 0, :, 0:256])
    q = z_q[:, :128] * csq_ref[:, :128] + z_q[:, 128:] * csq_ref[:, 128:]
    z_k = mm(ohk, tab_ref[0, 0, :, 256:512])
    k = z_k[:, :128] * csk_ref[:, :128] + z_k[:, 128:] * csk_ref[:, 128:]
    v = mm(ohk, tab_ref[0, 0, :, 512:640])
    return q, k.astype(BF16), v.astype(BF16)


def attn_fwd_kernel(len_ref, ohk_ref, ohq_ref, tab_ref, csk_ref, csq_ref, o_ref, lse_ref):
    seq_len = len_ref[pl.program_id(0)]
    q, k, v = expand_qkv(ohk_ref, ohq_ref, tab_ref, csk_ref, csq_ref)
    low = lax.broadcasted_iota(jnp.int32, (QLEN, 128), 1) < HDIM
    key_ok = lax.broadcasted_iota(jnp.int32, (QLEN, SEQ), 1) < seq_len
    outs, stats = [], []
    for head in range(2):
        q_h = jnp.where(low if head == 0 else jnp.logical_not(low), q, 0.0).astype(BF16)
        s = jnp.where(key_ok, mm(q_h, k, ((1,), (1,))), NEG_BIG)
        top = jnp.max(s, axis=-1, keepdims=True)
        e = jnp.exp(s - top)
        total = jnp.sum(e, axis=-1, keepdims=True)
        outs.append(mm(e.astype(BF16), v) / total)
        stats.append(jnp.broadcast_to(top + jnp.log(total), (QLEN, 128)))
    o_ref[0] = jnp.where(low, outs[0], outs[1]).astype(BF16)
    lse_ref[0] = jnp.where(low, stats[0], stats[1])


def attn_bwd_kernel(len_ref, ohk_ref, ohq_ref, tab_ref, csk_ref, csq_ref, do_ref, lse_ref, s_ref):
    seq_len = len_ref[pl.program_id(0)]
    q, k, v = expand_qkv(ohk_ref, ohq_ref, tab_ref, csk_ref, csq_ref)
    d_o = do_ref[0]
    low = lax.broadcasted_iota(jnp.int32, (QLEN, 128), 1) < HDIM
    key_ok = lax.broadcasted_iota(jnp.int32, (QLEN, SEQ), 1) < seq_len
    dv, dk, dqs = None, None, []
    for head in range(2):
        mine = low if head == 0 else jnp.logical_not(low)
        q_h = jnp.where(mine, q, 0.0).astype(BF16)
        do_h = jnp.where(mine, d_o, jnp.zeros_like(d_o))
        s = mm(q_h, k, ((1,), (1,)))
        p = jnp.where(key_ok, jnp.exp(s - lse_ref[0, :, HDIM * head:HDIM * head + 1]), 0.0)
        t = p * mm(do_h, v, ((1,), (1,)))
        ds = (t - p * jnp.sum(t, axis=-1, keepdims=True)).astype(BF16)
        dv_h = mm(p.astype(BF16), do_h, ((0,), (0,)))
        dk_h = mm(ds, q_h, ((0,), (0,)))
        dv = dv_h if dv is None else dv + dv_h
        dk = dk_h if dk is None else dk + dk_h
        dqs.append(mm(ds, k))
    dq = jnp.where(low, dqs[0], dqs[1])
    ohk = ohk_ref[0]
    ohq = ohq_ref[0]
    top = ((0,), (0,))
    s_ref[0, 0, :, 0:128] = mm(ohq, (dq * csq_ref[:, :128]).astype(BF16), top)[:ROWS]
    s_ref[0, 0, :, 128:256] = mm(ohq, (dq * csq_ref[:, 128:]).astype(BF16), top)[:ROWS]
    s_ref[0, 0, :, 256:384] = mm(ohk, (dk * csk_ref[:, :128]).astype(BF16), top)[:ROWS]
    s_ref[0, 0, :, 384:512] = mm(ohk, (dk * csk_ref[:, 128:]).astype(BF16), top)[:ROWS]
    s_ref[0, 0, :, 512:640] = mm(ohk, dv.astype(BF16), top)[:ROWS]


def attn_specs():
    return [
        pl.BlockSpec(memory_space=pltpu.SMEM),
        pl.BlockSpec((1, SEQ, 128), lambda b, j: (b, 0, 0)),
        pl.BlockSpec((1, QLEN, 128), lambda b, j: (b, 0, 0)),
        pl.BlockSpec((1, 1, 128, 640), lambda b, j: (b, j, 0, 0)),
        pl.BlockSpec((SEQ, 256), lambda b, j: (0, 0)),
        pl.BlockSpec((QLEN, 256), lambda b, j: (0, 0)),
    ]


def row_spec():
    return pl.BlockSpec((1, QLEN, 128), lambda b, j: (b, 0, j))


def attn_fwd(lengths, ohk, ohq, tab, csk, csq):
    return pl.pallas_call(
        attn_fwd_kernel, grid=(2, PAIRS), in_specs=attn_specs(), out_specs=[row_spec(), row_spec()],
        out_shape=[jax.ShapeDtypeStruct((2, QLEN, DIM), BF16), jax.ShapeDtypeStruct((2, QLEN, DIM), F32)],
        cost_estimate=pl.CostEstimate(flops=12_000_000_000, bytes_accessed=12_000_000, transcendentals=10_000_000),
        name='attn_fwd')(lengths, ohk, ohq, tab, csk, csq)


def attn_bwd(lengths, ohk, ohq, tab, csk, csq, d_o, lse):
    return pl.pallas_call(
        attn_bwd_kernel, grid=(2, PAIRS), in_specs=attn_specs() + [row_spec(), row_spec()],
        out_specs=pl.BlockSpec((1, 1, ROWS, 640), lambda b, j: (b, j, 0, 0)),
        out_shape=jax.ShapeDtypeStruct((2, PAIRS, ROWS, 640), F32),
        cost_estimate=pl.CostEstimate(flops=30_000_000_000, bytes_accessed=15_000_000, transcendentals=10_000_000),
        name='attn_bwd')(lengths, ohk, ohq, tab, csk, csq, d_o, lse)


def rot_half(z_in):
    return jnp.concatenate([-z_in[..., HDIM // 2:], z_in[..., :HDIM // 2]], axis=-1)


def rot_half_t(z_in):
    return jnp.concatenate([z_in[..., HDIM // 2:], -z_in[..., :HDIM // 2]], axis=-1)


def split3(z_in):
    hi = lax.reduce_precision(z_in, 8, 7)
    rest = z_in - hi
    mid = lax.reduce_precision(rest, 8, 7)
    return jnp.concatenate([hi.astype(BF16), mid.astype(BF16), (rest - mid).astype(BF16)], axis=1)


def build_tab(t_all):
    q = t_all[:, :, 0] * HDIM ** -0.5
    k = t_all[:, :, 1]
    v = t_all[:, :, 2]

    def pairs(z_in):
        return z_in.reshape(2, VOCAB, PAIRS, 128)
    wide = jnp.concatenate([pairs(q), pairs(rot_half(q)), pairs(k), pairs(rot_half(k))], axis=-1)
    wide = split3(wide)
    v_hi = jnp.pad(pairs(v).astype(BF16), ((0, 0), (0, 2 * VOCAB), (0, 0), (0, 0)))
    full = jnp.concatenate([wide, v_hi], axis=-1)
    full = jnp.pad(full, ((0, 0), (0, 128 - 3 * VOCAB), (0, 0), (0, 0)))
    return jnp.swapaxes(full, 1, 2)


def one_hot3(tok):
    lanes = jnp.arange(128)
    return ((tok[..., None] == lanes % VOCAB) & (lanes < 3 * VOCAB)).astype(BF16)


def all_sum(small, axes):
    for axis, size in axes:
        step = 1
        while step < size:
            small = small + lax.ppermute(small, axis, [(i, i ^ step) for i in range(size)])
            step *= 2
    return small


def solution(mesh):
    mesh4 = Mesh(mesh.devices.reshape(4, 4, 4, 2), ('x', 'z', 'y', 'c'))

    def local_step(tokens, lengths, embed_table, layer_vecs, w_qkv, w_out, w_up, b_up, w_down, grad_out):
        xi = lax.axis_index('x')
        ci = lax.axis_index('c')
        chip = lax.axis_index('z') * 4 + lax.axis_index('y')
        fi = chip * 2 + ci
        wq_loc = lax.dynamic_slice_in_dim(w_qkv, 5 * xi, 5, axis=2).reshape(ROWS, 960)
        qkv_w = lax.all_gather(wq_loc, FSDP, axis=0, tiled=True)
        packed = jnp.concatenate([layer_vecs.reshape(360), b_up, jnp.zeros((504,), F32)]).reshape(8, 128)
        packed = lax.all_gather(packed, FSDP, axis=0, tiled=True).reshape(32, 1024)
        vecs = packed[:, :360].reshape(32, 9, ROWS).transpose(1, 0, 2).reshape(9, DIM)
        up_b = lax.dynamic_index_in_dim(packed[:, 360:520].reshape(16, 2, 160), ci, axis=1, keepdims=False).reshape(2560)
        tok_all = lax.all_gather(tokens, 'x', axis=1, tiled=True)
        up_loc = w_up.reshape(ROWS, 16, 2, 160)
        up_mine = lax.dynamic_index_in_dim(up_loc, ci, axis=2, keepdims=False).reshape(ROWS, 2560)
        up_send = lax.dynamic_index_in_dim(up_loc, 1 - ci, axis=2, keepdims=False).reshape(ROWS, 2560)
        up_recv = lax.ppermute(up_send, 'c', SWAP)
        up_pair = jnp.concatenate([jnp.where(ci == 0, up_mine, up_recv), jnp.where(ci == 0, up_recv, up_mine)], axis=0)
        shard = jnp.concatenate([up_pair[:, :DIM], up_pair[:, DIM:], w_down, w_out], axis=0)
        gathered = lax.all_gather(shard, CHIP, axis=0, tiled=False)
        grad_own = grad_out.reshape(2 * QLEN, DIM)
        grad2 = jnp.concatenate([grad_own, lax.ppermute(grad_own, 'c', SWAP)], axis=0)

        positions = jnp.arange(SEQ)
        tok_eff = jnp.where(positions[None, :] < lengths[:, None], tok_all, MASK_ID)
        tok_own = lax.dynamic_slice_in_dim(tok_eff, xi * QLEN, QLEN, axis=1)
        mask_count = jnp.sum((tok_all == MASK_ID).astype(F32), axis=1)
        drop_scale = (1.0 - TRAIN_RATIO) / (1.0 - mask_count / lengths.astype(F32))
        ohk = one_hot3(tok_eff)
        ohq = one_hot3(tok_own)
        oh_own = ohq[:, :, :VOCAB]
        row_scale = jnp.where(jnp.arange(VOCAB)[None, :] == MASK_ID, 0.0, drop_scale[:, None])
        e_rows = embed_table.astype(F32)[None] * row_scale[:, :, None]
        xhat1, inv1 = ln_stats(e_rows)
        h_rows = (xhat1 * vecs[0] + vecs[1]).astype(BF16).reshape(2 * VOCAB, DIM)
        t_loc = mm(h_rows, qkv_w)
        t_all = lax.all_gather(t_loc, 'x', axis=0, tiled=False)
        t_all = t_all.reshape(4, 2, VOCAB, 3, 5, HDIM).transpose(1, 2, 3, 0, 4, 5).reshape(2, VOCAB, 3, HEADS, HDIM)
        t_all = t_all + vecs[2:5].reshape(3, HEADS, HDIM)
        tab = build_tab(t_all)
        inv_freq = 1.0 / (ROPE_BASE ** (jnp.arange(0, HDIM, 2, dtype=F32) / HDIM))
        angles = positions.astype(F32)[:, None] * inv_freq[None, :]
        csk = jnp.concatenate([jnp.tile(jnp.cos(angles), (1, 4)), jnp.tile(jnp.sin(angles), (1, 4))], axis=1)
        csq = lax.dynamic_slice_in_dim(csk, xi * QLEN, QLEN, axis=0)

        attn_o, lse = attn_fwd(lengths, ohk, ohq, tab, csk, csq)
        attn_o, gathered = lax.optimization_barrier((attn_o, gathered))
        up_w0 = gathered[:, 0:80].reshape(DIM, DIM)
        up_w1 = gathered[:, 80:160].reshape(DIM, DIM)
        down_w = gathered[:, 160:320].reshape(2 * DIM, DIM)
        out_mine = gathered[:, 320:360]
        out_recv = lax.ppermute(out_mine, 'c', SWAP)
        out_w = jnp.stack([jnp.where(ci == 0, out_mine, out_recv), jnp.where(ci == 0, out_recv, out_mine)], axis=1).reshape(DIM, DIM)
        attn_o2 = attn_o.reshape(2 * QLEN, DIM)
        keep_own = jnp.where(tok_own == MASK_ID, 0.0, drop_scale[:, None])
        embedded = jnp.einsum('bsv,vd->bsd', oh_own, embed_table, preferred_element_type=F32) * keep_own[:, :, None]
        x1 = embedded.reshape(2 * QLEN, DIM) + mm(attn_o2, out_w) + vecs[5]
        xhat2, inv2 = ln_stats(x1)
        nm = (xhat2 * vecs[6] + vecs[7]).astype(BF16)
        nm2 = jnp.concatenate([nm, lax.ppermute(nm, 'c', SWAP)], axis=0)
        up_lin = jnp.concatenate([mm(nm2, up_w0), mm(nm2, up_w1)], axis=1) + up_b
        cdf = 0.5 * (1.0 + lax.erf(up_lin * 0.7071067811865476))
        gelu_b = (up_lin * cdf).astype(BF16)
        slope = cdf + up_lin * (0.3989422804014327 * jnp.exp(-0.5 * up_lin * up_lin))
        down2 = mm(gelu_b, down_w)
        down_got = lax.ppermute(down2[2 * QLEN:], 'c', SWAP)
        layer_out = (x1 + down2[:2 * QLEN] + down_got + vecs[8]).astype(BF16).reshape(2, QLEN, DIM)

        d_down = mm(gelu_b, grad2, ((0,), (0,)))
        d_up_lin = mm(grad2, down_w, ((1,), (1,))) * slope
        d_up_b = d_up_lin.astype(BF16)
        d_up = mm(nm2, d_up_b, ((0,), (0,)))
        d_nm2 = mm(d_up_b[:, :DIM], up_w0, ((1,), (1,))) + mm(d_up_b[:, DIM:], up_w1, ((1,), (1,)))
        d_nm = d_nm2[:2 * QLEN] + lax.ppermute(d_nm2[2 * QLEN:], 'c', SWAP)
        grad32 = grad_own.astype(F32)
        d_resid = grad32 + ln_back(d_nm, vecs[6], xhat2, inv2)
        d_resid_b = d_resid.astype(BF16)
        d_outw = mm(attn_o2, d_resid_b, ((0,), (0,)))
        d_attn_b = mm(d_resid_b, out_w, ((1,), (1,))).astype(BF16)
        s_tab = attn_bwd(lengths, ohk, ohq, tab, csk, csq, d_attn_b.reshape(2, QLEN, DIM), lse)

        s_tab = jnp.swapaxes(s_tab[:, :, :VOCAB], 1, 2)

        def heads(z_in):
            return z_in.reshape(2, VOCAB, HEADS, HDIM)
        s_q = (heads(s_tab[..., 0:128]) + rot_half_t(heads(s_tab[..., 128:256]))) * HDIM ** -0.5
        s_k = heads(s_tab[..., 256:384]) + rot_half_t(heads(s_tab[..., 384:512]))
        s_v = heads(s_tab[..., 512:640])
        s_all = jnp.stack([s_q, s_k, s_v], axis=2)
        d_bqkv = jnp.sum(s_all, axis=(0, 1)).reshape(3, DIM)
        s_x = s_all.reshape(2 * VOCAB, 3, 4, 5, HDIM).transpose(2, 0, 1, 3, 4).reshape(4, 2 * VOCAB, 960)
        s_mine = lax.dynamic_index_in_dim(s_x, xi, axis=0, keepdims=False)
        for hop in range(1, 4):
            part = lax.dynamic_index_in_dim(s_x, (xi + hop) % 4, axis=0, keepdims=False)
            s_mine = s_mine + lax.ppermute(part, 'x', [(i, (i + hop) % 4) for i in range(4)])
        d_qkvw = lax.dot_general(h_rows.astype(F32), s_mine, (((0,), (0,)), ((), ())), precision=HIGH, preferred_element_type=F32)
        d_h = lax.dot_general(s_mine, qkv_w.astype(F32), (((1,), (1,)), ((), ())), precision=HIGH, preferred_element_type=F32)
        d_h = d_h.reshape(2, VOCAB, DIM)
        d_e = ln_back(d_h, vecs[0], xhat1, inv1)
        d_e = d_e + jnp.einsum('bsv,bsd->bvd', oh_own, d_resid_b.reshape(2, QLEN, DIM), preferred_element_type=F32)
        d_table = jnp.sum(d_e * row_scale[:, :, None], axis=0)
        d_up_bias = jnp.sum(d_up_lin, axis=0).reshape(1, 2, DIM)
        d_up_bias = jnp.where(jnp.arange(2)[:, None, None] == ci, d_up_bias, 0.0).reshape(4, DIM)
        small = jnp.concatenate([
            d_table,
            jnp.sum(d_h * xhat1, axis=(0, 1))[None], jnp.sum(d_h, axis=(0, 1))[None], d_bqkv,
            jnp.sum(d_resid, axis=0)[None], jnp.sum(d_nm * xhat2, axis=0)[None], jnp.sum(d_nm, axis=0)[None],
            jnp.sum(grad32, axis=0)[None], d_up_bias, jnp.zeros((2, DIM), F32)], axis=0)
        small = all_sum(small, (('c', 2), ('x', 4), ('y', 4), ('z', 4)))
        d_vecs = lax.dynamic_slice(small, (VOCAB, fi * ROWS), (9, ROWS))
        d_bup_half = lax.dynamic_slice_in_dim(small, VOCAB + 9 + 2 * ci, 2, axis=0).reshape(2560)
        d_bup = lax.dynamic_slice_in_dim(d_bup_half, chip * 160, 160, axis=0)

        r_down = all_sum(lax.psum_scatter(d_down, CHIP, scatter_dimension=0, tiled=True), (('x', 4),))
        r_up = all_sum(lax.psum_scatter(d_up, CHIP, scatter_dimension=0, tiled=True), (('x', 4),))
        d_oq = jnp.concatenate([d_outw, d_qkvw, jnp.zeros((DIM, PADW), F32)], axis=1).reshape(16, 2, ROWS, DIM + 960 + PADW)
        oq_keep = lax.dynamic_index_in_dim(d_oq, ci, axis=1, keepdims=False)
        oq_give = lax.dynamic_index_in_dim(d_oq, 1 - ci, axis=1, keepdims=False)
        d_oq = oq_keep + lax.ppermute(oq_give, 'c', SWAP)
        r_oq = lax.psum_scatter(d_oq, CHIP, scatter_dimension=0, tiled=False)
        r_out = all_sum(r_oq[:, :DIM], (('x', 4),))
        r_qkv = lax.all_gather(r_oq[:, DIM:DIM + 960], 'x', axis=0, tiled=False)
        up_keep = lax.dynamic_slice_in_dim(r_up, ci * ROWS, ROWS, axis=0)
        up_give = lax.dynamic_slice_in_dim(r_up, (1 - ci) * ROWS, ROWS, axis=0)
        up_got = lax.ppermute(up_give, 'c', SWAP)
        r_up = jnp.stack([jnp.where(ci == 0, up_keep, up_got).reshape(ROWS, 16, 160),
                          jnp.where(ci == 0, up_got, up_keep).reshape(ROWS, 16, 160)], axis=2).reshape(ROWS, 5120)
        r_qkv = r_qkv.reshape(4, ROWS, 3, 5, HDIM).transpose(1, 2, 0, 3, 4).reshape(ROWS, 3, HEADS, HDIM)
        return layer_out, small[:VOCAB], d_vecs, r_qkv, r_out, r_up, d_bup, r_down

    in_specs = (P(FSDP, 'x'), P(FSDP), P(), P(None, FSDP), P(FSDP, None, None, None), P(FSDP, None), P(FSDP, None), P(FSDP), P(FSDP, None), P(FSDP, 'x', None))
    out_specs = (P(FSDP, 'x', None), P(), P(None, FSDP), P(FSDP, None, None, None), P(FSDP, None), P(FSDP, None), P(FSDP), P(FSDP, None))
    return jax.shard_map(local_step, mesh=mesh4, in_specs=in_specs, out_specs=out_specs, check_vma=False)
```

```python
import functools

import jax
import jax.numpy as jnp
from jax import lax
from jax.experimental import pallas as pl
from jax.experimental.pallas import tpu as pltpu
from jax.sharding import Mesh, PartitionSpec as P

MASK_ID = 32
VOCAB = 33
LN_EPS = 1e-5
ROPE_BASE = 10000.0
TRAIN_RATIO = 0.15 * 0.8
NEG_BIG = -1e30
SEQ = 1024
QLEN = 256
HEADS = 20
HDIM = 64
PAIRS = HEADS // 2
DIM = HEADS * HDIM
ROWS = 40
F32 = jnp.float32
BF16 = jnp.bfloat16
SWAP = [(0, 1), (1, 0)]
CHIP = ('z', 'y')
FSDP = ('z', 'y', 'c')
QCOLS = 1024
MESH = pl.DeviceIdType.MESH
LO, HI, ALL = range(3)
NT = ((1,), (1,))
TN = ((0,), (0,))
LANES = 128
HALF = HDIM // 2
FFH = 2 * DIM
TOK = 2 * QLEN
HALF_D = DIM // 2
COST = pl.CostEstimate(flops=20_000_000_000, bytes_accessed=15_000_000, transcendentals=10_000_000)
HIGH = lax.Precision.HIGHEST


def mm(a, b, dims=((1,), (0,))):
    return lax.dot_general(a, b, (dims, ((), ())), preferred_element_type=F32)


def ln_stats(z_in):
    row_mean = jnp.mean(z_in, axis=-1, keepdims=True)
    centered = z_in - row_mean
    row_var = jnp.mean(centered * centered, axis=-1, keepdims=True)
    inv = lax.rsqrt(row_var + LN_EPS)
    return centered * inv, inv


def ln_back(d_out, gain, xhat, inv):
    d_hat = d_out * gain
    m1 = jnp.mean(d_hat, axis=-1, keepdims=True)
    m2 = jnp.mean(d_hat * xhat, axis=-1, keepdims=True)
    return inv * (d_hat - m1 - xhat * m2)


def rot_half(z_in, sign):
    lane = lax.broadcasted_iota(jnp.int32, z_in.shape, 1)
    down, up = pltpu.roll(z_in, LANES - HALF, 1), pltpu.roll(z_in, HALF, 1)
    return jnp.where(lane % HDIM < HALF, -sign * down, sign * up)


def split3(z_in):
    hi = z_in.astype(BF16).astype(F32)
    rest = z_in - hi
    mid = rest.astype(BF16).astype(F32)
    return jnp.concatenate([hi, mid, rest - mid, jnp.zeros((LANES - 3 * ROWS, z_in.shape[1]), F32)], axis=0).astype(BF16)


def expand_qkv(ohk_ref, ohq_ref, tq_ref, tk_ref, tv_ref, csk_ref, csq_ref):
    ohk = ohk_ref[0]
    t_q = tq_ref[0] * HDIM ** -0.5
    z_q = mm(ohq_ref[0], split3(jnp.concatenate([t_q, rot_half(t_q, 1.0)], axis=1)))
    q = z_q[:, :LANES] * csq_ref[:, :LANES] + z_q[:, LANES:] * csq_ref[:, LANES:]
    t_k = tk_ref[0]
    z_k = mm(ohk, split3(jnp.concatenate([t_k, rot_half(t_k, 1.0)], axis=1)))
    k = z_k[:, :LANES] * csk_ref[:, :LANES] + z_k[:, LANES:] * csk_ref[:, LANES:]
    t_v = jnp.concatenate([tv_ref[0], jnp.zeros((LANES - ROWS, LANES), F32)], axis=0)
    v = mm(ohk, t_v.astype(BF16))
    return q, k.astype(BF16), v.astype(BF16)


def attn_fwd_kernel(len_ref, ohk_ref, ohq_ref, tq_ref, tk_ref, tv_ref, csk_ref, csq_ref, o_ref, lse_ref):
    seq_len = len_ref[pl.program_id(0)]
    q, k, v = expand_qkv(ohk_ref, ohq_ref, tq_ref, tk_ref, tv_ref, csk_ref, csq_ref)
    low = lax.broadcasted_iota(jnp.int32, (QLEN, LANES), 1) < HDIM
    key_ok = lax.broadcasted_iota(jnp.int32, (QLEN, SEQ), 1) < seq_len
    outs, stats = [], []
    for head in range(2):
        q_h = jnp.where(low if head == 0 else jnp.logical_not(low), q, 0.0).astype(BF16)
        s = jnp.where(key_ok, mm(q_h, k, NT), NEG_BIG)
        top = jnp.max(s, axis=-1, keepdims=True)
        e = jnp.exp(s - top)
        total = jnp.sum(e, axis=-1, keepdims=True)
        outs.append(mm(e.astype(BF16), v) / total)
        stats.append(jnp.broadcast_to(top + jnp.log(total), (QLEN, LANES)))
    o_ref[0] = jnp.where(low, outs[0], outs[1]).astype(BF16)
    lse_ref[0] = jnp.where(low, stats[0], stats[1])


def attn_bwd_kernel(len_ref, ohk_ref, ohq_ref, tq_ref, tk_ref, tv_ref, csk_ref, csq_ref, do_ref, lse_ref, sq_ref, sk_ref, sv_ref):
    seq_len = len_ref[pl.program_id(0)]
    q, k, v = expand_qkv(ohk_ref, ohq_ref, tq_ref, tk_ref, tv_ref, csk_ref, csq_ref)
    d_o = do_ref[0]
    low = lax.broadcasted_iota(jnp.int32, (QLEN, LANES), 1) < HDIM
    key_ok = lax.broadcasted_iota(jnp.int32, (QLEN, SEQ), 1) < seq_len
    dv, dk, dqs = None, None, []
    for head in range(2):
        mine = low if head == 0 else jnp.logical_not(low)
        q_h = jnp.where(mine, q, 0.0).astype(BF16)
        do_h = jnp.where(mine, d_o, jnp.zeros_like(d_o))
        s = mm(q_h, k, NT)
        p = jnp.where(key_ok, jnp.exp(s - lse_ref[0, :, HDIM * head:HDIM * head + 1]), 0.0)
        t = p * mm(do_h, v, NT)
        ds = (t - p * jnp.sum(t, axis=-1, keepdims=True)).astype(BF16)
        dv_h = mm(p.astype(BF16), do_h, TN)
        dk_h = mm(ds, q_h, TN)
        dv = dv_h if dv is None else dv + dv_h
        dk = dk_h if dk is None else dk + dk_h
        dqs.append(mm(ds, k))
    dq = jnp.where(low, dqs[0], dqs[1])
    ohk = ohk_ref[0]
    ohq = ohq_ref[0]
    top = TN
    real = lax.broadcasted_iota(jnp.int32, (ROWS, LANES), 0) < VOCAB

    def by_token(onehot, d_in):
        return jnp.where(real, mm(onehot, d_in.astype(BF16), top)[:ROWS], 0.0)
    s_q = by_token(ohq, dq * csq_ref[:, :LANES]) + rot_half(by_token(ohq, dq * csq_ref[:, LANES:]), -1.0)
    sq_ref[0] = s_q * HDIM ** -0.5
    sk_ref[0] = by_token(ohk, dk * csk_ref[:, :LANES]) + rot_half(by_token(ohk, dk * csk_ref[:, LANES:]), -1.0)
    sv_ref[0] = by_token(ohk, dv)


def tab_spec():
    return pl.BlockSpec((1, ROWS, LANES), lambda b, j: (b, 0, j))


def attn_specs():
    return [
        pl.BlockSpec(memory_space=pltpu.SMEM),
        pl.BlockSpec((1, SEQ, LANES), lambda b, j: (b, 0, 0)),
        pl.BlockSpec((1, QLEN, LANES), lambda b, j: (b, 0, 0)),
        tab_spec(),
        tab_spec(),
        tab_spec(),
        pl.BlockSpec((SEQ, 256), lambda b, j: (0, 0)),
        pl.BlockSpec((QLEN, 256), lambda b, j: (0, 0)),
    ]


def row_spec():
    return pl.BlockSpec((1, QLEN, LANES), lambda b, j: (b, 0, j))


def attn_fwd(lengths, ohk, ohq, tq, tk, tv, csk, csq):
    return pl.pallas_call(
        attn_fwd_kernel, grid=(2, PAIRS), in_specs=attn_specs(), out_specs=[row_spec(), row_spec()],
        out_shape=[jax.ShapeDtypeStruct((2, QLEN, DIM), BF16), jax.ShapeDtypeStruct((2, QLEN, DIM), F32)],
        cost_estimate=COST,
        name='attn_fwd')(lengths, ohk, ohq, tq, tk, tv, csk, csq)


def attn_bwd(lengths, ohk, ohq, tq, tk, tv, csk, csq, d_o, lse):
    return pl.pallas_call(
        attn_bwd_kernel, grid=(2, PAIRS), in_specs=attn_specs() + [row_spec(), row_spec()],
        out_specs=[tab_spec()] * 3, out_shape=[jax.ShapeDtypeStruct((2, ROWS, DIM), F32)] * 3,
        cost_estimate=COST,
        name='attn_bwd')(lengths, ohk, ohq, tq, tk, tv, csk, csq, d_o, lse)


class Ring:
    def __init__(self, axis, ports):
        self.me = lax.axis_index(axis)
        self.axis, self.ports = axis, ports
        self.right = lax.rem(self.me + 1, 4)
        self.left = lax.rem(self.me + 3, 4)
        self.far = lax.rem(self.me + 2, 4)
        self.open = []

    def send(self, src, dst, to):
        copy = remote(src, dst, next(self.ports), {self.axis: to})
        copy.start()
        self.open.append(copy)
        return copy

    def drain(self):
        for copy in self.open:
            copy.wait_send()
        self.open = []

    def rs_start(self, chunk, bufs):
        self.chunk = chunk
        self.b1, self.b2, self.b3, self.b4, self.b5, self.b6 = bufs
        self.m1 = self.send(chunk(self.far, LO), self.b1, self.right)
        self.m3 = self.send(chunk(self.far, HI), self.b3, self.left)
        self.m2 = self.send(chunk(self.right, HI), self.b2, self.right)
        self.m4 = self.send(chunk(self.left, LO), self.b4, self.left)

    def rs_mid(self):
        self.m1.wait_recv()
        self.b1[...] += self.chunk(self.right, LO)[...]
        self.m5 = self.send(self.b1, self.b5, self.right)
        self.m3.wait_recv()
        self.b3[...] += self.chunk(self.left, HI)[...]
        self.m6 = self.send(self.b3, self.b6, self.left)

    def rs_end(self):
        self.m4.wait_recv()
        self.m5.wait_recv()
        low = self.chunk(self.me, LO)[...] + self.b4[...] + self.b5[...]
        self.m2.wait_recv()
        self.m6.wait_recv()
        high = self.chunk(self.me, HI)[...] + self.b2[...] + self.b6[...]
        self.drain()
        return low, high

    def ag_start(self, slot):
        self.slot = slot
        self.a1 = self.send(slot(self.me, ALL), slot(self.me, ALL), self.right)
        self.a2 = self.send(slot(self.me, ALL), slot(self.me, ALL), self.left)

    def ag_mid(self):
        self.a1.wait_recv()
        self.a3 = self.send(self.slot(self.left, LO), self.slot(self.left, LO), self.right)
        self.a2.wait_recv()
        self.a4 = self.send(self.slot(self.right, HI), self.slot(self.right, HI), self.left)

    def ag_end(self):
        self.a3.wait_recv()
        self.a4.wait_recv()
        self.drain()


def meet():
    barrier = pltpu.get_barrier_semaphore()
    for axis in ('x', 'z', 'y'):
        me = lax.axis_index(axis)
        for step in (1, 3):
            pl.semaphore_signal(barrier, inc=1, device_id={axis: lax.rem(me + step, 4)}, device_id_type=MESH)
    pl.semaphore_signal(barrier, inc=1, device_id={'c': 1 - lax.axis_index('c')}, device_id_type=MESH)
    pl.semaphore_wait(barrier, 7)


def ports_of(sends, recvs):
    return ((sends.at[i], recvs.at[i]) for i in range(sends.shape[0]))


def remote(src, dst, port, target):
    return pltpu.make_async_remote_copy(src_ref=src, dst_ref=dst, send_sem=port[0], recv_sem=port[-1], device_id=target, device_id_type=MESH)


def core_copy(src, dst, ports):
    return remote(src, dst, next(ports), {'c': 1 - lax.axis_index('c')})


CUT = 24
HALF_W = 1152
WIDE = DIM + QCOLS


def half_rows(half):
    return pl.ds(0, CUT) if half == LO else pl.ds(CUT, ROWS - CUT)


def ring_bufs(lead, width):
    return [pltpu.VMEM(lead + (CUT if i in (0, 3, 4) else ROWS - CUT, width), F32) for i in range(6)]


def oq_kernel(d_out_ref, d_qkv_ref, out_ref, qkv_ref, acc, one_a, one_b, gath, *rest):
    bufs, ports = [rest[6 * i:6 * i + 6] for i in range(4)], ports_of(*rest[-2:])
    ci = lax.axis_index('c')
    meet()
    first = core_copy(d_out_ref.at[:, 1 - ci], acc.at[:, :, pl.ds(0, DIM)], ports)
    second = core_copy(d_qkv_ref.at[:, 1 - ci], acc.at[:, :, pl.ds(DIM, QCOLS)], ports)
    first.start()
    second.start()
    first.wait_recv()

    def add_out(i, carry):
        acc[i, :, :DIM] += d_out_ref[i, ci]
        return carry
    lax.fori_loop(0, 16, add_out, 0)
    second.wait_recv()

    def add_qkv(i, carry):
        acc[i, :, DIM:] += d_qkv_ref[i, ci]
        return carry
    lax.fori_loop(0, 16, add_qkv, 0)
    grid = acc.reshape(4, 4, ROWS, WIDE)
    ya = Ring('y', ports)
    zb = Ring('z', ports)
    ya.rs_start(lambda k, h: grid.at[:, k, half_rows(h), pl.ds(0, HALF_W)], bufs[0])
    zb.rs_start(lambda k, h: grid.at[k, :, half_rows(h), pl.ds(HALF_W, HALF_W)], bufs[1])
    ya.rs_mid()
    zb.rs_mid()
    one_a[:, :CUT], one_a[:, CUT:] = ya.rs_end()
    za = Ring('z', ports)
    za.rs_start(lambda k, h: one_a.at[k, half_rows(h)], bufs[2])
    one_b[:, :CUT], one_b[:, CUT:] = zb.rs_end()
    yb = Ring('y', ports)
    yb.rs_start(lambda k, h: one_b.at[k, half_rows(h)], bufs[3])
    za.rs_mid()
    yb.rs_mid()
    xr = Ring('x', ports)
    low, high = za.rs_end()
    gath[xr.me, :CUT, :HALF_W] = low
    gath[xr.me, CUT:, :HALF_W] = high
    low, high = yb.rs_end()
    gath[xr.me, :CUT, HALF_W:] = low
    gath[xr.me, CUT:, HALF_W:] = high
    xr.ag_start(lambda k, h: gath.at[k] if h == ALL else gath.at[k, half_rows(h)])
    xr.ag_mid()
    xr.ag_end()
    out_ref[...] = (gath[0, :, :DIM] + gath[1, :, :DIM]) + (gath[2, :, :DIM] + gath[3, :, :DIM])
    for k in range(4):
        qkv_ref[:, QCOLS * k:QCOLS * (k + 1)] = gath[k, :, DIM:]
    first.wait_send()
    second.wait_send()


def vmem(n):
    return [pl.BlockSpec(memory_space=pltpu.VMEM)] * n


def reduce_oq(d_out, d_qkv):
    return pl.pallas_call(
        oq_kernel, in_specs=vmem(2), out_specs=vmem(2),
        out_shape=[jax.ShapeDtypeStruct((ROWS, DIM), F32), jax.ShapeDtypeStruct((ROWS, 4 * QCOLS), F32)],
        scratch_shapes=[pltpu.VMEM((16, ROWS, WIDE), F32), pltpu.VMEM((4, ROWS, HALF_W), F32), pltpu.VMEM((4, ROWS, HALF_W), F32),
                        pltpu.VMEM((4, ROWS, WIDE), F32)]
        + ring_bufs((4,), HALF_W) + ring_bufs((4,), HALF_W) + ring_bufs((), HALF_W) + ring_bufs((), HALF_W)
        + [pltpu.SemaphoreType.DMA((30,)), pltpu.SemaphoreType.DMA((30,))],
        compiler_params=pltpu.CompilerParams(collective_id=1, has_side_effects=True, vmem_limit_bytes=56 * 1024 * 1024),
        cost_estimate=COST,
        name='reduce_oq')(d_out, d_qkv)


SMALL = 48
UP_R = 80


def last_kernel(up_ref, down_ref, small_ref, up_out, down_out, small_out, pair, sum_y, sum_z, sum_x, *rest):
    bufs, ports = [rest[6 * i:6 * i + 6] for i in range(2)], ports_of(*rest[-2:])
    ci = lax.axis_index('c')
    meet()

    def up_rows(half):
        return pl.ds(40 * half, 40)
    swap = core_copy(small_ref, pair, ports)
    swap.start()
    xu = Ring('x', ports)
    xd = Ring('x', ports)
    xu.rs_start(lambda k, h: up_ref.at[k, up_rows(h)], bufs[0])
    xd.rs_start(lambda k, h: down_ref.at[k, half_rows(h)], bufs[1])
    swap.wait_recv()
    both = small_ref[...] + pair[...]
    mine = jnp.where(ci == 0, both[:, 0:HALF_D], both[:, HALF_D:1280])

    def gather(ref):
        return lambda k, h: ref.at[k] if h == ALL else ref.at[k, pl.ds(24 * h, 24)]

    def total(ref):
        return (ref[0] + ref[1]) + (ref[2] + ref[3])
    ys = Ring('y', ports)
    sum_y[ys.me] = mine
    ys.ag_start(gather(sum_y))
    xu.rs_mid()
    xd.rs_mid()
    ys.ag_mid()
    ys.ag_end()
    zs = Ring('z', ports)
    sum_z[zs.me] = total(sum_y)
    zs.ag_start(gather(sum_z))
    low, high = xu.rs_end()
    up_out[xu.me, 0:40] = low
    up_out[xu.me, 40:80] = high
    gu = Ring('x', ports)
    gu.ag_start(lambda k, h: up_out.at[k] if h == ALL else up_out.at[k, up_rows(h)])
    low, high = xd.rs_end()
    down_out[xd.me, :CUT] = low
    down_out[xd.me, CUT:] = high
    gd = Ring('x', ports)
    gd.ag_start(lambda k, h: down_out.at[k] if h == ALL else down_out.at[k, half_rows(h)])
    zs.ag_mid()
    zs.ag_end()
    xs = Ring('x', ports)
    sum_x[xs.me] = total(sum_z)
    xs.ag_start(gather(sum_x))
    gu.ag_mid()
    gd.ag_mid()
    xs.ag_mid()
    xs.ag_end()
    small_out[ci] = total(sum_x)
    back = core_copy(small_out.at[ci], small_out.at[ci], ports)
    back.start()
    gu.ag_end()
    gd.ag_end()
    back.wait_recv()
    back.wait_send()
    swap.wait_send()


def reduce_last(up, down, small):
    up_bufs = [pltpu.VMEM((40, HALF_D), F32) for _ in range(6)]
    return pl.pallas_call(
        last_kernel, in_specs=vmem(3), out_specs=vmem(3),
        out_shape=[jax.ShapeDtypeStruct((4, UP_R, HALF_D), F32), jax.ShapeDtypeStruct((4, ROWS, DIM), F32), jax.ShapeDtypeStruct((2, SMALL, HALF_D), F32)],
        scratch_shapes=[pltpu.VMEM((SMALL, DIM), F32)] + [pltpu.VMEM((4, SMALL, HALF_D), F32)] * 3 + up_bufs + ring_bufs((), DIM)
        + [pltpu.SemaphoreType.DMA((34,)), pltpu.SemaphoreType.DMA((34,))],
        compiler_params=pltpu.CompilerParams(collective_id=2, has_side_effects=True, vmem_limit_bytes=40 * 1024 * 1024),
        name='reduce_last')(up, down, small)


def one_hot3(tok):
    lanes = jnp.arange(LANES)
    return ((tok[..., None] == lanes % ROWS) & (lanes < 3 * ROWS)).astype(BF16)


def solution(mesh):
    mesh4 = Mesh(mesh.devices.reshape(4, 4, 4, 2), ('x', 'z', 'y', 'c'))

    def local_step(tokens, lengths, embed_table, layer_vecs, w_qkv, w_out, w_up, b_up, w_down, grad_out):
        xi = lax.axis_index('x')
        ci = lax.axis_index('c')
        chip = lax.axis_index('z') * 4 + lax.axis_index('y')
        fi = chip * 2 + ci
        wq_loc = lax.dynamic_slice_in_dim(jnp.pad(w_qkv.reshape(ROWS, 3 * DIM), ((0, 0), (0, 256))), QCOLS * xi, QCOLS, axis=1)
        qkv_w = lax.all_gather(wq_loc, FSDP, axis=0, tiled=True)
        packed = jnp.concatenate([layer_vecs.reshape(360), b_up, jnp.zeros((504,), F32)]).reshape(8, LANES)
        packed = lax.all_gather(packed, FSDP, axis=0, tiled=True).reshape(32, 1024)
        vecs = packed[:, :360].reshape(32, 9, ROWS).transpose(1, 0, 2).reshape(9, DIM)
        up_b = lax.dynamic_index_in_dim(packed[:, 360:520].reshape(16, 2, 160), ci, axis=1, keepdims=False).reshape(FFH)
        tok_all = lax.all_gather(tokens, 'x', axis=1, tiled=True)
        up_loc = w_up.reshape(ROWS, 16, 2, 160)
        up_mine = lax.dynamic_index_in_dim(up_loc, ci, axis=2, keepdims=False).reshape(ROWS, FFH)
        up_send = lax.dynamic_index_in_dim(up_loc, 1 - ci, axis=2, keepdims=False).reshape(ROWS, FFH)
        up_recv = lax.ppermute(up_send, 'c', SWAP)
        up_pair = jnp.concatenate([jnp.where(ci == 0, up_mine, up_recv), jnp.where(ci == 0, up_recv, up_mine)], axis=0)
        shard = jnp.concatenate([up_pair[:, :DIM], up_pair[:, DIM:], w_down, w_out], axis=0)
        gathered = lax.all_gather(shard, CHIP, axis=0, tiled=False)
        grad_own = grad_out.reshape(TOK, DIM)
        grad2 = jnp.concatenate([grad_own, lax.ppermute(grad_own, 'c', SWAP)], axis=0)

        positions = jnp.arange(SEQ)
        tok_eff = jnp.where(positions[None, :] < lengths[:, None], tok_all, MASK_ID)
        tok_own = lax.dynamic_slice_in_dim(tok_eff, xi * QLEN, QLEN, axis=1)
        mask_count = jnp.sum((tok_all == MASK_ID).astype(F32), axis=1)
        drop_scale = (1.0 - TRAIN_RATIO) / (1.0 - mask_count / lengths.astype(F32))
        ohk = one_hot3(tok_eff)
        ohq = one_hot3(tok_own)
        oh_own = ohq[:, :, :VOCAB]
        row_scale = jnp.where(jnp.arange(VOCAB)[None, :] == MASK_ID, 0.0, drop_scale[:, None])
        e_rows = embed_table.astype(F32)[None] * row_scale[:, :, None]
        xhat1, inv1 = ln_stats(e_rows)
        h_rows = (xhat1 * vecs[0] + vecs[1]).astype(BF16)
        h_rows = jnp.pad(h_rows, ((0, 0), (0, ROWS - VOCAB), (0, 0))).reshape(2 * ROWS, DIM)
        t_loc = mm(h_rows, qkv_w)
        t_all = jnp.zeros((2 * ROWS, 4 * QCOLS), F32)
        for hop in range(4):
            part = lax.ppermute(t_loc, 'x', [(i, (i + hop) % 4) for i in range(4)]) if hop else t_loc
            t_all = lax.dynamic_update_slice_in_dim(t_all, part, QCOLS * ((xi + 4 - hop) % 4), axis=1)
        t_all = (t_all[:, :3 * DIM] + vecs[2:5].reshape(1, 3 * DIM)).reshape(2, ROWS, 3 * DIM)
        tabs = (t_all[:, :, :DIM], t_all[:, :, DIM:2 * DIM], t_all[:, :, 2 * DIM:])
        inv_freq = 1.0 / (ROPE_BASE ** (jnp.arange(0, HDIM, 2, dtype=F32) / HDIM))
        angles = positions.astype(F32)[:, None] * inv_freq[None, :]
        csk = jnp.concatenate([jnp.tile(jnp.cos(angles), (1, 4)), jnp.tile(jnp.sin(angles), (1, 4))], axis=1)
        csq = lax.dynamic_slice_in_dim(csk, xi * QLEN, QLEN, axis=0)

        attn_o, lse = attn_fwd(lengths, ohk, ohq, *tabs, csk, csq)
        attn_o, gathered = lax.optimization_barrier((attn_o, gathered))
        up_w0 = gathered[:, 0:80].reshape(DIM, DIM)
        up_w1 = gathered[:, 80:160].reshape(DIM, DIM)
        down_w = gathered[:, 160:320].reshape(2 * DIM, DIM)
        out_mine = gathered[:, 320:360]
        out_recv = lax.ppermute(out_mine, 'c', SWAP)
        out_w = jnp.stack([jnp.where(ci == 0, out_mine, out_recv), jnp.where(ci == 0, out_recv, out_mine)], axis=1).reshape(DIM, DIM)
        attn_o2 = attn_o.reshape(TOK, DIM)
        keep_own = jnp.where(tok_own == MASK_ID, 0.0, drop_scale[:, None])
        embedded = jnp.einsum('bsv,vd->bsd', oh_own, embed_table, preferred_element_type=F32) * keep_own[:, :, None]
        x1 = embedded.reshape(TOK, DIM) + mm(attn_o2, out_w) + vecs[5]
        xhat2, inv2 = ln_stats(x1)
        nm = (xhat2 * vecs[6] + vecs[7]).astype(BF16)
        nm2 = jnp.concatenate([nm, lax.ppermute(nm, 'c', SWAP)], axis=0)
        up_lin = jnp.concatenate([mm(nm2, up_w0), mm(nm2, up_w1)], axis=1) + up_b
        cdf = 0.5 * (1.0 + lax.erf(up_lin * 0.7071067811865476))
        gelu_b = (up_lin * cdf).astype(BF16)
        slope = cdf + up_lin * (0.3989422804014327 * jnp.exp(-0.5 * up_lin * up_lin))
        down2 = mm(gelu_b, down_w)
        down_got = lax.ppermute(down2[TOK:], 'c', SWAP)
        layer_out = (x1 + down2[:TOK] + down_got + vecs[8]).astype(BF16).reshape(2, QLEN, DIM)

        d_down = mm(gelu_b, grad2, TN)
        d_up_lin = mm(grad2, down_w, NT) * slope
        d_up_b = d_up_lin.astype(BF16)
        d_up = mm(nm2, d_up_b, TN)
        d_nm2 = mm(d_up_b[:, :DIM], up_w0, NT) + mm(d_up_b[:, DIM:], up_w1, NT)
        d_nm = d_nm2[:TOK] + lax.ppermute(d_nm2[TOK:], 'c', SWAP)
        grad32 = grad_own.astype(F32)
        d_resid = grad32 + ln_back(d_nm, vecs[6], xhat2, inv2)
        d_resid_b = d_resid.astype(BF16)
        d_outw = mm(attn_o2, d_resid_b, TN)
        d_attn_b = mm(d_resid_b, out_w, NT).astype(BF16)
        s_q, s_k, s_v = attn_bwd(lengths, ohk, ohq, *tabs, csk, csq, d_attn_b.reshape(2, QLEN, DIM), lse)

        d_bqkv = jnp.stack([jnp.sum(part, axis=(0, 1)) for part in (s_q, s_k, s_v)])
        s_all = jnp.concatenate([s_q, s_k, s_v, jnp.zeros((2, ROWS, 256), F32)], axis=2).reshape(2 * ROWS, 4 * QCOLS)
        s_mine = lax.dynamic_slice_in_dim(s_all, QCOLS * xi, QCOLS, axis=1)
        for hop in range(1, 4):
            part = lax.dynamic_slice_in_dim(s_all, QCOLS * ((xi + hop) % 4), QCOLS, axis=1)
            s_mine = s_mine + lax.ppermute(part, 'x', [(i, (i + hop) % 4) for i in range(4)])
        d_qkvw = lax.dot_general(h_rows.astype(F32), s_mine, (TN, ((), ())), precision=HIGH)
        d_h = lax.dot_general(s_mine, qkv_w.astype(F32), (NT, ((), ())), precision=HIGH)
        d_h = d_h.reshape(2, ROWS, DIM)[:, :VOCAB]
        d_e = ln_back(d_h, vecs[0], xhat1, inv1)
        d_e = d_e + jnp.einsum('bsv,bsd->bvd', oh_own, d_resid_b.reshape(2, QLEN, DIM), preferred_element_type=F32)
        d_table = jnp.sum(d_e * row_scale[:, :, None], axis=0)
        d_up_bias = jnp.sum(d_up_lin, axis=0).reshape(1, 2, DIM)
        d_up_bias = jnp.where(jnp.arange(2)[:, None, None] == ci, d_up_bias, 0.0).reshape(4, DIM)
        small = jnp.concatenate([
            d_table,
            jnp.sum(d_h * xhat1, axis=(0, 1))[None], jnp.sum(d_h, axis=(0, 1))[None], d_bqkv,
            jnp.sum(d_resid, axis=0)[None], jnp.sum(d_nm * xhat2, axis=0)[None], jnp.sum(d_nm, axis=0)[None],
            jnp.sum(grad32, axis=0)[None], d_up_bias, jnp.zeros((2, DIM), F32)], axis=0)
        r_out, r_qkv = reduce_oq(d_outw.reshape(16, 2, ROWS, DIM), d_qkvw.reshape(16, 2, ROWS, QCOLS))
        r_down = lax.psum_scatter(d_down, CHIP, scatter_dimension=0, tiled=True)
        r_up = lax.psum_scatter(d_up, CHIP, scatter_dimension=0, tiled=True)
        small, r_out = lax.optimization_barrier((small, r_out))
        r_up, r_down, small = reduce_last(r_up.reshape(2 * ROWS, 4, HALF_D).transpose(1, 0, 2), r_down.reshape(4, ROWS, DIM), small)
        r_up = r_up.transpose(1, 0, 2).reshape(2 * ROWS, FFH)
        r_down = r_down.reshape(160, DIM)
        small = small.transpose(1, 0, 2).reshape(SMALL, DIM)
        d_vecs = lax.dynamic_slice(small, (VOCAB, fi * ROWS), (9, ROWS))
        d_bup_half = lax.dynamic_slice_in_dim(small, VOCAB + 9 + 2 * ci, 2, axis=0).reshape(FFH)
        d_bup = lax.dynamic_slice_in_dim(d_bup_half, chip * 160, 160, axis=0)

        up_keep = lax.dynamic_slice_in_dim(r_up, ci * ROWS, ROWS, axis=0)
        up_give = lax.dynamic_slice_in_dim(r_up, (1 - ci) * ROWS, ROWS, axis=0)
        up_got = lax.ppermute(up_give, 'c', SWAP)
        r_up = jnp.stack([jnp.where(ci == 0, up_keep, up_got).reshape(ROWS, 16, 160),
                          jnp.where(ci == 0, up_got, up_keep).reshape(ROWS, 16, 160)], axis=2).reshape(ROWS, 5120)
        r_qkv = r_qkv[:, :3 * DIM].reshape(ROWS, 3, HEADS, HDIM)
        return layer_out, small[:VOCAB], d_vecs, r_qkv, r_out, r_up, d_bup, r_down

    in_specs = (P(FSDP, 'x'), P(FSDP), P(), P(None, FSDP), P(FSDP), P(FSDP), P(FSDP), P(FSDP), P(FSDP), P(FSDP, 'x'))
    out_specs = (P(FSDP, 'x'), P(), P(None, FSDP), P(FSDP), P(FSDP), P(FSDP), P(FSDP), P(FSDP))
    return jax.shard_map(local_step, mesh=mesh4, in_specs=in_specs, out_specs=out_specs, check_vma=False)
```

```python
import functools

import jax
import jax.numpy as jnp
from jax import lax
from jax.experimental import pallas as pl
from jax.experimental.pallas import tpu as pltpu
from jax.sharding import Mesh, PartitionSpec as P

MASK_ID = 32
VOCAB = 33
LN_EPS = 1e-5
ROPE_BASE = 10000.0
TRAIN_RATIO = 0.15 * 0.8
NEG_BIG = -1e30
SEQ = 1024
QLEN = 256
HEADS = 20
HDIM = 64
PAIRS = HEADS // 2
DIM = HEADS * HDIM
ROWS = 40
F32 = jnp.float32
BF16 = jnp.bfloat16
SWAP = [(0, 1), (1, 0)]
CHIP = ('z', 'y')
FSDP = ('z', 'y', 'c')
QCOLS = 1024
MESH = pl.DeviceIdType.MESH
LO, HI, ALL = range(3)
NT = ((1,), (1,))
TN = ((0,), (0,))
LANES = 128
HALF = HDIM // 2
FFH = 2 * DIM
TOK = 2 * QLEN
HALF_D = DIM // 2
COST = pl.CostEstimate(flops=20_000_000_000, bytes_accessed=15_000_000, transcendentals=10_000_000)
HIGH = lax.Precision.HIGHEST


def mm(a, b, dims=((1,), (0,))):
    return lax.dot_general(a, b, (dims, ((), ())), preferred_element_type=F32)


def ln_stats(z_in):
    row_mean = jnp.mean(z_in, axis=-1, keepdims=True)
    centered = z_in - row_mean
    row_var = jnp.mean(centered * centered, axis=-1, keepdims=True)
    inv = lax.rsqrt(row_var + LN_EPS)
    return centered * inv, inv


def ln_back(d_out, gain, xhat, inv):
    d_hat = d_out * gain
    m1 = jnp.mean(d_hat, axis=-1, keepdims=True)
    m2 = jnp.mean(d_hat * xhat, axis=-1, keepdims=True)
    return inv * (d_hat - m1 - xhat * m2)


def rot_half(z_in, sign):
    lane = lax.broadcasted_iota(jnp.int32, z_in.shape, 1)
    down, up = pltpu.roll(z_in, LANES - HALF, 1), pltpu.roll(z_in, HALF, 1)
    return jnp.where(lane % HDIM < HALF, -sign * down, sign * up)


def split3(z_in):
    hi = z_in.astype(BF16).astype(F32)
    rest = z_in - hi
    mid = rest.astype(BF16).astype(F32)
    return jnp.concatenate([hi, mid, rest - mid, jnp.zeros((LANES - 3 * ROWS, z_in.shape[1]), F32)], axis=0).astype(BF16)


def expand_qkv(ohk_ref, ohq_ref, tq_ref, tk_ref, tv_ref, csk_ref, csq_ref):
    ohk = ohk_ref[0]
    t_q = tq_ref[0] * HDIM ** -0.5
    z_q = mm(ohq_ref[0], split3(jnp.concatenate([t_q, rot_half(t_q, 1.0)], axis=1)))
    q = z_q[:, :LANES] * csq_ref[:, :LANES] + z_q[:, LANES:] * csq_ref[:, LANES:]
    t_k = tk_ref[0]
    z_k = mm(ohk, split3(jnp.concatenate([t_k, rot_half(t_k, 1.0)], axis=1)))
    k = z_k[:, :LANES] * csk_ref[:, :LANES] + z_k[:, LANES:] * csk_ref[:, LANES:]
    t_v = jnp.concatenate([tv_ref[0], jnp.zeros((LANES - ROWS, LANES), F32)], axis=0)
    v = mm(ohk, t_v.astype(BF16))
    return q, k.astype(BF16), v.astype(BF16)


def head_masks():
    low = lax.broadcasted_iota(jnp.int32, (QLEN, LANES), 1) < HDIM
    return low, jnp.logical_not(low)


def key_mask(seq_len):
    return lax.broadcasted_iota(jnp.int32, (SEQ, QLEN), 0) < seq_len


def head_cols(head):
    return slice(HDIM * head, HDIM * (head + 1))


def attn_fwd_kernel(len_ref, ohk_ref, ohq_ref, tq_ref, tk_ref, tv_ref, csk_ref, csq_ref, o_ref, lse_ref):
    q, k, v = expand_qkv(ohk_ref, ohq_ref, tq_ref, tk_ref, tv_ref, csk_ref, csq_ref)
    key_ok = key_mask(len_ref[pl.program_id(0)])
    v_t = v.T
    outs = []
    for head, mine in enumerate(head_masks()):
        q_h = jnp.where(mine, q, 0.0).astype(BF16)
        s = jnp.where(key_ok, mm(k, q_h, NT), NEG_BIG)
        top = jnp.max(s, axis=0, keepdims=True)
        e = jnp.exp(s - top)
        total = jnp.sum(e, axis=0, keepdims=True)
        outs.append(mm(v_t[head_cols(head)], e.astype(BF16)) / total)
        lse_ref[0, 0, head:head + 1, :] = top + jnp.log(total)
    o_ref[0] = jnp.concatenate(outs, axis=0).T.astype(BF16)


def attn_bwd_kernel(len_ref, ohk_ref, ohq_ref, tq_ref, tk_ref, tv_ref, csk_ref, csq_ref, okt_ref, oqt_ref, do_ref, lse_ref, sq_ref, sk_ref, sv_ref):
    q, k, v = expand_qkv(ohk_ref, ohq_ref, tq_ref, tk_ref, tv_ref, csk_ref, csq_ref)
    d_o = do_ref[0]
    key_ok = key_mask(len_ref[pl.program_id(0)])
    k_t = k.T
    dv, dk, dqs = None, None, []
    for head, mine in enumerate(head_masks()):
        q_h = jnp.where(mine, q, 0.0).astype(BF16)
        do_h = jnp.where(mine, d_o, jnp.zeros_like(d_o))
        p = jnp.where(key_ok, jnp.exp(mm(k, q_h, NT) - lse_ref[0, 0, head:head + 1, :]), 0.0)
        t = p * mm(v, do_h, NT)
        ds = (t - p * jnp.sum(t, axis=0, keepdims=True)).astype(BF16)
        dv_h = mm(p.astype(BF16), do_h)
        dk_h = mm(ds, q_h)
        dv = dv_h if dv is None else dv + dv_h
        dk = dk_h if dk is None else dk + dk_h
        dqs.append(mm(k_t[head_cols(head)], ds))
    dq = jnp.concatenate(dqs, axis=0).T

    def by_token(onehot_t, d_in):
        return mm(onehot_t, d_in.astype(BF16))
    s_q = by_token(oqt_ref[0], jnp.concatenate([dq * csq_ref[:, :LANES], dq * csq_ref[:, LANES:]], axis=1))
    sq_ref[0] = (s_q[:, :LANES] + rot_half(s_q[:, LANES:], -1.0)) * HDIM ** -0.5
    s_k = by_token(okt_ref[0], jnp.concatenate([dk * csk_ref[:, :LANES], dk * csk_ref[:, LANES:]], axis=1))
    sk_ref[0] = s_k[:, :LANES] + rot_half(s_k[:, LANES:], -1.0)
    sv_ref[0] = by_token(okt_ref[0], dv)


def tab_spec():
    return pl.BlockSpec((1, ROWS, LANES), lambda b, j: (b, 0, j))


def attn_specs():
    return [
        pl.BlockSpec(memory_space=pltpu.SMEM),
        pl.BlockSpec((1, SEQ, LANES), lambda b, j: (b, 0, 0)),
        pl.BlockSpec((1, QLEN, LANES), lambda b, j: (b, 0, 0)),
        tab_spec(),
        tab_spec(),
        tab_spec(),
        pl.BlockSpec((SEQ, 256), lambda b, j: (0, 0)),
        pl.BlockSpec((QLEN, 256), lambda b, j: (0, 0)),
    ]


def row_spec():
    return pl.BlockSpec((1, QLEN, LANES), lambda b, j: (b, 0, j))


def lse_spec():
    return pl.BlockSpec((1, 1, 8, QLEN), lambda b, j: (b, j, 0, 0))


def attn_fwd(lengths, ohk, ohq, tq, tk, tv, csk, csq):
    return pl.pallas_call(
        attn_fwd_kernel, grid=(2, PAIRS), in_specs=attn_specs(), out_specs=[row_spec(), lse_spec()],
        out_shape=[jax.ShapeDtypeStruct((2, QLEN, DIM), BF16), jax.ShapeDtypeStruct((2, PAIRS, 8, QLEN), F32)],
        cost_estimate=COST,
        name='attn_fwd')(lengths, ohk, ohq, tq, tk, tv, csk, csq)


def attn_bwd(lengths, ohk, ohq, tq, tk, tv, csk, csq, okt, oqt, d_o, lse):
    return pl.pallas_call(
        attn_bwd_kernel, grid=(2, PAIRS), in_specs=attn_specs() + [pl.BlockSpec((1, ROWS, SEQ), lambda b, j: (b, 0, 0)), pl.BlockSpec((1, ROWS, QLEN), lambda b, j: (b, 0, 0)), row_spec(), lse_spec()],
        out_specs=[tab_spec()] * 3, out_shape=[jax.ShapeDtypeStruct((2, ROWS, DIM), F32)] * 3,
        cost_estimate=COST,
        name='attn_bwd')(lengths, ohk, ohq, tq, tk, tv, csk, csq, okt, oqt, d_o, lse)


class Ring:
    def __init__(self, axis, ports):
        self.me = lax.axis_index(axis)
        self.axis, self.ports = axis, ports
        self.right = lax.rem(self.me + 1, 4)
        self.left = lax.rem(self.me + 3, 4)
        self.far = lax.rem(self.me + 2, 4)
        self.open = []

    def send(self, src, dst, to):
        copy = remote(src, dst, next(self.ports), {self.axis: to})
        copy.start()
        self.open.append(copy)
        return copy

    def drain(self):
        for copy in self.open:
            copy.wait_send()
        self.open = []

    def rs_start(self, chunk, bufs):
        self.chunk = chunk
        self.b1, self.b2, self.b3, self.b4, self.b5, self.b6 = bufs
        self.m1 = self.send(chunk(self.far, LO), self.b1, self.right)
        self.m3 = self.send(chunk(self.far, HI), self.b3, self.left)
        self.m2 = self.send(chunk(self.right, HI), self.b2, self.right)
        self.m4 = self.send(chunk(self.left, LO), self.b4, self.left)

    def rs_mid(self):
        self.m1.wait_recv()
        self.b1[...] += self.chunk(self.right, LO)[...]
        self.m5 = self.send(self.b1, self.b5, self.right)
        self.m3.wait_recv()
        self.b3[...] += self.chunk(self.left, HI)[...]
        self.m6 = self.send(self.b3, self.b6, self.left)

    def rs_end(self):
        self.m4.wait_recv()
        self.m5.wait_recv()
        low = self.chunk(self.me, LO)[...] + self.b4[...] + self.b5[...]
        self.m2.wait_recv()
        self.m6.wait_recv()
        high = self.chunk(self.me, HI)[...] + self.b2[...] + self.b6[...]
        self.drain()
        return low, high

    def ag_start(self, slot, own=None, split=True):
        self.slot, self.split = slot, split
        home = slot(self.me, ALL)
        own = home if own is None else own
        self.a1 = self.send(own, home, self.right)
        self.a2 = self.send(own, home, self.left)

    def ag_mid(self):
        self.a1.wait_recv()
        part = self.slot(self.left, LO if self.split else ALL)
        self.a3 = self.send(part, part, self.right)
        self.a2.wait_recv()
        if self.split:
            part = self.slot(self.right, HI)
            self.a4 = self.send(part, part, self.left)

    def ag_end(self):
        self.a3.wait_recv()
        if self.split:
            self.a4.wait_recv()
        self.drain()


def meet():
    barrier = pltpu.get_barrier_semaphore()
    for axis in ('x', 'z', 'y'):
        me = lax.axis_index(axis)
        for step in (1, 3):
            pl.semaphore_signal(barrier, inc=1, device_id={axis: lax.rem(me + step, 4)}, device_id_type=MESH)
    pl.semaphore_signal(barrier, inc=1, device_id={'c': 1 - lax.axis_index('c')}, device_id_type=MESH)
    pl.semaphore_wait(barrier, 7)


def ports_of(sends, recvs):
    return ((sends.at[i], recvs.at[i]) for i in range(sends.shape[0]))


def remote(src, dst, port, target):
    return pltpu.make_async_remote_copy(src_ref=src, dst_ref=dst, send_sem=port[0], recv_sem=port[-1], device_id=target, device_id_type=MESH)


def core_copy(src, dst, ports):
    return remote(src, dst, next(ports), {'c': 1 - lax.axis_index('c')})


CUT = 24
HALF_W = 1152
WIDE = DIM + QCOLS


def half_rows(half):
    return pl.ds(0, CUT) if half == LO else pl.ds(CUT, ROWS - CUT)


def ring_bufs(lead, width):
    return [pltpu.VMEM(lead + (CUT if i in (0, 3, 4) else ROWS - CUT, width), F32) for i in range(6)]


def oq_kernel(d_out_ref, d_qkv_ref, out_ref, qkv_ref, acc, one_a, one_b, gath, *rest):
    bufs, ports = [rest[6 * i:6 * i + 6] for i in range(4)], ports_of(*rest[-2:])
    ci = lax.axis_index('c')
    meet()
    first = core_copy(d_out_ref.at[:, 1 - ci], acc.at[:, :, pl.ds(0, DIM)], ports)
    second = core_copy(d_qkv_ref.at[:, 1 - ci], acc.at[:, :, pl.ds(DIM, QCOLS)], ports)
    first.start()
    second.start()
    first.wait_recv()

    def add_out(i, carry):
        acc[i, :, :DIM] += d_out_ref[i, ci]
        return carry
    lax.fori_loop(0, 16, add_out, 0)
    second.wait_recv()

    def add_qkv(i, carry):
        acc[i, :, DIM:] += d_qkv_ref[i, ci]
        return carry
    lax.fori_loop(0, 16, add_qkv, 0)
    grid = acc.reshape(4, 4, ROWS, WIDE)
    ya = Ring('y', ports)
    zb = Ring('z', ports)
    ya.rs_start(lambda k, h: grid.at[:, k, half_rows(h), pl.ds(0, HALF_W)], bufs[0])
    zb.rs_start(lambda k, h: grid.at[k, :, half_rows(h), pl.ds(HALF_W, HALF_W)], bufs[1])
    ya.rs_mid()
    zb.rs_mid()
    one_a[:, :CUT], one_a[:, CUT:] = ya.rs_end()
    za = Ring('z', ports)
    za.rs_start(lambda k, h: one_a.at[k, half_rows(h)], bufs[2])
    one_b[:, :CUT], one_b[:, CUT:] = zb.rs_end()
    yb = Ring('y', ports)
    yb.rs_start(lambda k, h: one_b.at[k, half_rows(h)], bufs[3])
    za.rs_mid()
    yb.rs_mid()
    xr = Ring('x', ports)
    low, high = za.rs_end()
    gath[xr.me, :CUT, :HALF_W] = low
    gath[xr.me, CUT:, :HALF_W] = high
    low, high = yb.rs_end()
    gath[xr.me, :CUT, HALF_W:] = low
    gath[xr.me, CUT:, HALF_W:] = high
    xr.ag_start(lambda k, h: gath.at[k] if h == ALL else gath.at[k, half_rows(h)])
    xr.ag_mid()
    xr.ag_end()
    out_ref[...] = (gath[0, :, :DIM] + gath[1, :, :DIM]) + (gath[2, :, :DIM] + gath[3, :, :DIM])
    for k in range(4):
        qkv_ref[:, QCOLS * k:QCOLS * (k + 1)] = gath[k, :, DIM:]
    first.wait_send()
    second.wait_send()


def vmem(n):
    return [pl.BlockSpec(memory_space=pltpu.VMEM)] * n


def reduce_oq(d_out, d_qkv):
    return pl.pallas_call(
        oq_kernel, in_specs=vmem(2), out_specs=vmem(2),
        out_shape=[jax.ShapeDtypeStruct((ROWS, DIM), F32), jax.ShapeDtypeStruct((ROWS, 4 * QCOLS), F32)],
        scratch_shapes=[pltpu.VMEM((16, ROWS, WIDE), F32), pltpu.VMEM((4, ROWS, HALF_W), F32), pltpu.VMEM((4, ROWS, HALF_W), F32),
                        pltpu.VMEM((4, ROWS, WIDE), F32)]
        + ring_bufs((4,), HALF_W) + ring_bufs((4,), HALF_W) + ring_bufs((), HALF_W) + ring_bufs((), HALF_W)
        + [pltpu.SemaphoreType.DMA((30,)), pltpu.SemaphoreType.DMA((30,))],
        compiler_params=pltpu.CompilerParams(collective_id=1, has_side_effects=True, vmem_limit_bytes=56 * 1024 * 1024),
        cost_estimate=COST,
        name='reduce_oq')(d_out, d_qkv)


def first_kernel(wq_ref, wo_ref, pack_ref, tok_ref, gq, go, gp, gt, sends, recvs):
    ports = ports_of(sends, recvs)
    ci = lax.axis_index('c')
    y1, z1, yp, xt = Ring('y', ports), Ring('z', ports), Ring('y', ports), Ring('x', ports)
    y2, z2, zp = Ring('y', ports), Ring('z', ports), Ring('z', ports)
    yi, zi = y1.me, z1.me
    meet()
    y1.ag_start(lambda k, h: gq.at[zi, k, ci] if h == ALL else gq.at[zi, k, ci, :, pl.ds(QCOLS // 2 * h, QCOLS // 2)], wq_ref)
    z1.ag_start(lambda k, h: go.at[k, yi, ci] if h == ALL else go.at[k, yi, ci, :, pl.ds(HALF_D * h, HALF_D)], wo_ref)
    yp.ag_start(lambda k, h: gp.at[zi, k, ci], pack_ref, False)
    xt.ag_start(lambda k, h: gt.at[k], tok_ref, False)
    gq[zi, yi, ci] = wq_ref[...]
    go[zi, yi, ci] = wo_ref[...]
    gp[zi, yi, ci] = pack_ref[...]
    gt[xt.me] = tok_ref[...]
    stage = (y1, z1, yp, xt)
    for ring in stage:
        ring.ag_mid()
    for ring in stage:
        ring.ag_end()
    z2.ag_start(lambda k, h: gq.at[k, :, ci] if h == ALL else gq.at[k, pl.ds(2 * h, 2), ci])
    y2.ag_start(lambda k, h: go.at[:, k, ci] if h == ALL else go.at[pl.ds(2 * h, 2), k, ci])
    zp.ag_start(lambda k, h: gp.at[k, :, ci], None, False)
    stage = (z2, y2, zp)
    for ring in stage:
        ring.ag_mid()
    for ring in stage:
        ring.ag_end()
    swaps = [core_copy(ref.at[:, :, ci], ref.at[:, :, ci], ports) for ref in (gq, go, gp)]
    for swap in swaps:
        swap.start()
    for swap in swaps:
        swap.wait_recv()
        swap.wait_send()


def gather_first(wq, wo, pack, tok):
    return pl.pallas_call(
        first_kernel, in_specs=vmem(4), out_specs=vmem(4),
        out_shape=[jax.ShapeDtypeStruct((4, 4, 2) + wq.shape, BF16), jax.ShapeDtypeStruct((4, 4, 2) + wo.shape, BF16),
                   jax.ShapeDtypeStruct((4, 4, 2) + pack.shape, F32), jax.ShapeDtypeStruct((4,) + tok.shape, jnp.int32)],
        scratch_shapes=[pltpu.SemaphoreType.DMA((28,)), pltpu.SemaphoreType.DMA((28,))],
        compiler_params=pltpu.CompilerParams(collective_id=3, has_side_effects=True, vmem_limit_bytes=24 * 1024 * 1024),
        cost_estimate=COST, name='gather_first')(wq, wo, pack, tok)


SMALL = 48
UP_R = 80


def last_kernel(up_ref, down_ref, small_ref, up_out, down_out, small_out, pair, sum_y, sum_z, sum_x, *rest):
    bufs, ports = [rest[6 * i:6 * i + 6] for i in range(2)], ports_of(*rest[-2:])
    ci = lax.axis_index('c')
    meet()

    def up_rows(half):
        return pl.ds(40 * half, 40)
    swap = core_copy(small_ref, pair, ports)
    swap.start()
    xu = Ring('x', ports)
    xd = Ring('x', ports)
    xu.rs_start(lambda k, h: up_ref.at[k, up_rows(h)], bufs[0])
    xd.rs_start(lambda k, h: down_ref.at[k, half_rows(h)], bufs[1])
    swap.wait_recv()
    both = small_ref[...] + pair[...]
    mine = jnp.where(ci == 0, both[:, 0:HALF_D], both[:, HALF_D:1280])

    def gather(ref):
        return lambda k, h: ref.at[k] if h == ALL else ref.at[k, pl.ds(24 * h, 24)]

    def total(ref):
        return (ref[0] + ref[1]) + (ref[2] + ref[3])
    ys = Ring('y', ports)
    sum_y[ys.me] = mine
    ys.ag_start(gather(sum_y))
    xu.rs_mid()
    xd.rs_mid()
    ys.ag_mid()
    ys.ag_end()
    zs = Ring('z', ports)
    sum_z[zs.me] = total(sum_y)
    zs.ag_start(gather(sum_z))
    low, high = xu.rs_end()
    up_out[xu.me, 0:40] = low
    up_out[xu.me, 40:80] = high
    gu = Ring('x', ports)
    gu.ag_start(lambda k, h: up_out.at[k] if h == ALL else up_out.at[k, up_rows(h)])
    low, high = xd.rs_end()
    down_out[xd.me, :CUT] = low
    down_out[xd.me, CUT:] = high
    gd = Ring('x', ports)
    gd.ag_start(lambda k, h: down_out.at[k] if h == ALL else down_out.at[k, half_rows(h)])
    zs.ag_mid()
    zs.ag_end()
    xs = Ring('x', ports)
    sum_x[xs.me] = total(sum_z)
    xs.ag_start(gather(sum_x))
    gu.ag_mid()
    gd.ag_mid()
    xs.ag_mid()
    xs.ag_end()
    small_out[ci] = total(sum_x)
    back = core_copy(small_out.at[ci], small_out.at[ci], ports)
    back.start()
    gu.ag_end()
    gd.ag_end()
    back.wait_recv()
    back.wait_send()
    swap.wait_send()


def reduce_last(up, down, small):
    up_bufs = [pltpu.VMEM((40, HALF_D), F32) for _ in range(6)]
    return pl.pallas_call(
        last_kernel, in_specs=vmem(3), out_specs=vmem(3),
        out_shape=[jax.ShapeDtypeStruct((4, UP_R, HALF_D), F32), jax.ShapeDtypeStruct((4, ROWS, DIM), F32), jax.ShapeDtypeStruct((2, SMALL, HALF_D), F32)],
        scratch_shapes=[pltpu.VMEM((SMALL, DIM), F32)] + [pltpu.VMEM((4, SMALL, HALF_D), F32)] * 3 + up_bufs + ring_bufs((), DIM)
        + [pltpu.SemaphoreType.DMA((34,)), pltpu.SemaphoreType.DMA((34,))],
        compiler_params=pltpu.CompilerParams(collective_id=2, has_side_effects=True, vmem_limit_bytes=40 * 1024 * 1024),
        name='reduce_last')(up, down, small)


def one_hot3(tok):
    lanes = jnp.arange(LANES)
    return ((tok[..., None] == lanes % ROWS) & (lanes < 3 * ROWS)).astype(BF16)


def solution(mesh):
    mesh4 = Mesh(mesh.devices.reshape(4, 4, 4, 2), ('x', 'z', 'y', 'c'))

    def local_step(tokens, lengths, embed_table, layer_vecs, w_qkv, w_out, w_up, b_up, w_down, grad_out):
        xi = lax.axis_index('x')
        ci = lax.axis_index('c')
        chip = lax.axis_index('z') * 4 + lax.axis_index('y')
        fi = chip * 2 + ci
        wq_loc = lax.dynamic_slice_in_dim(jnp.pad(w_qkv.reshape(ROWS, 3 * DIM), ((0, 0), (0, 256))), QCOLS * xi, QCOLS, axis=1)
        packed = jnp.concatenate([layer_vecs.reshape(360), b_up, jnp.zeros((504,), F32)]).reshape(8, LANES)
        up_loc = w_up.reshape(ROWS, 16, 2, 160)
        up_mine = lax.dynamic_index_in_dim(up_loc, ci, axis=2, keepdims=False).reshape(ROWS, FFH)
        up_send = lax.dynamic_index_in_dim(up_loc, 1 - ci, axis=2, keepdims=False).reshape(ROWS, FFH)
        up_recv = lax.ppermute(up_send, 'c', SWAP)
        up_pair = jnp.concatenate([jnp.where(ci == 0, up_mine, up_recv), jnp.where(ci == 0, up_recv, up_mine)], axis=0)
        shard = jnp.concatenate([up_pair[:, :DIM], up_pair[:, DIM:], w_down], axis=0)
        shard, packed = lax.optimization_barrier((shard, packed))
        gathered = lax.all_gather(shard, CHIP, axis=0, tiled=False)
        qkv_w, out_w, packed, tok_all = gather_first(wq_loc, w_out, packed, tokens.reshape(4, LANES))
        qkv_w, out_w, packed = qkv_w.reshape(DIM, QCOLS), out_w.reshape(DIM, DIM), packed.reshape(32, 8 * LANES)
        tok_all = tok_all.reshape(4, 2, QLEN).transpose(1, 0, 2).reshape(2, SEQ)
        vecs = packed[:, :360].reshape(32, 9, ROWS).transpose(1, 0, 2).reshape(9, DIM)
        up_b = lax.dynamic_index_in_dim(packed[:, 360:520].reshape(16, 2, 160), ci, axis=1, keepdims=False).reshape(FFH)
        grad_own = grad_out.reshape(TOK, DIM)
        grad2 = jnp.concatenate([grad_own, lax.ppermute(grad_own, 'c', SWAP)], axis=0)

        positions = jnp.arange(SEQ)
        tok_eff = jnp.where(positions[None, :] < lengths[:, None], tok_all, MASK_ID)
        tok_own = lax.dynamic_slice_in_dim(tok_eff, xi * QLEN, QLEN, axis=1)
        mask_count = jnp.sum((tok_all == MASK_ID).astype(F32), axis=1)
        drop_scale = (1.0 - TRAIN_RATIO) / (1.0 - mask_count / lengths.astype(F32))
        ohk = one_hot3(tok_eff)
        ohq = one_hot3(tok_own)
        oh_own = ohq[:, :, :VOCAB]
        rows = jnp.arange(ROWS)[:, None]
        okt = (tok_eff[:, None, :] == rows).astype(BF16)
        oqt = (tok_own[:, None, :] == rows).astype(BF16)
        row_scale = jnp.where(jnp.arange(VOCAB)[None, :] == MASK_ID, 0.0, drop_scale[:, None])
        e_rows = embed_table.astype(F32)[None] * row_scale[:, :, None]
        xhat1, inv1 = ln_stats(e_rows)
        h_rows = (xhat1 * vecs[0] + vecs[1]).astype(BF16)
        h_rows = jnp.pad(h_rows, ((0, 0), (0, ROWS - VOCAB), (0, 0))).reshape(2 * ROWS, DIM)
        t_loc = mm(h_rows, qkv_w)
        t_all = jnp.zeros((2 * ROWS, 4 * QCOLS), F32)
        for hop in range(4):
            part = lax.ppermute(t_loc, 'x', [(i, (i + hop) % 4) for i in range(4)]) if hop else t_loc
            t_all = lax.dynamic_update_slice_in_dim(t_all, part, QCOLS * ((xi + 4 - hop) % 4), axis=1)
        t_all = (t_all[:, :3 * DIM] + vecs[2:5].reshape(1, 3 * DIM)).reshape(2, ROWS, 3 * DIM)
        tabs = (t_all[:, :, :DIM], t_all[:, :, DIM:2 * DIM], t_all[:, :, 2 * DIM:])
        inv_freq = 1.0 / (ROPE_BASE ** (jnp.arange(0, HDIM, 2, dtype=F32) / HDIM))
        angles = positions.astype(F32)[:, None] * inv_freq[None, :]
        csk = jnp.concatenate([jnp.tile(jnp.cos(angles), (1, 4)), jnp.tile(jnp.sin(angles), (1, 4))], axis=1)
        csq = lax.dynamic_slice_in_dim(csk, xi * QLEN, QLEN, axis=0)

        attn_o, lse = attn_fwd(lengths, ohk, ohq, *tabs, csk, csq)
        attn_o2 = attn_o.reshape(TOK, DIM)
        keep_own = jnp.where(tok_own == MASK_ID, 0.0, drop_scale[:, None])
        embedded = jnp.einsum('bsv,vd->bsd', oh_own, embed_table, preferred_element_type=F32) * keep_own[:, :, None]
        x1 = embedded.reshape(TOK, DIM) + mm(attn_o2, out_w) + vecs[5]
        xhat2, inv2 = ln_stats(x1)
        nm = (xhat2 * vecs[6] + vecs[7]).astype(BF16)
        nm2 = jnp.concatenate([nm, lax.ppermute(nm, 'c', SWAP)], axis=0)
        nm2, gathered = lax.optimization_barrier((nm2, gathered))
        up_w0 = gathered[:, 0:80].reshape(DIM, DIM)
        up_w1 = gathered[:, 80:160].reshape(DIM, DIM)
        down_w = gathered[:, 160:320].reshape(2 * DIM, DIM)
        up_lin = jnp.concatenate([mm(nm2, up_w0), mm(nm2, up_w1)], axis=1) + up_b
        cdf = 0.5 * (1.0 + lax.erf(up_lin * 0.7071067811865476))
        gelu_b = (up_lin * cdf).astype(BF16)
        slope = cdf + up_lin * (0.3989422804014327 * jnp.exp(-0.5 * up_lin * up_lin))
        down2 = mm(gelu_b, down_w)
        down_got = lax.ppermute(down2[TOK:], 'c', SWAP)
        layer_out = (x1 + down2[:TOK] + down_got + vecs[8]).astype(BF16).reshape(2, QLEN, DIM)

        d_down = mm(gelu_b, grad2, TN)
        d_up_lin = mm(grad2, down_w, NT) * slope
        d_up_b = d_up_lin.astype(BF16)
        d_up = mm(nm2, d_up_b, TN)
        d_nm2 = mm(d_up_b[:, :DIM], up_w0, NT) + mm(d_up_b[:, DIM:], up_w1, NT)
        d_nm = d_nm2[:TOK] + lax.ppermute(d_nm2[TOK:], 'c', SWAP)
        grad32 = grad_own.astype(F32)
        d_resid = grad32 + ln_back(d_nm, vecs[6], xhat2, inv2)
        d_resid_b = d_resid.astype(BF16)
        d_outw = mm(attn_o2, d_resid_b, TN)
        d_attn_b = mm(d_resid_b, out_w, NT).astype(BF16)
        s_q, s_k, s_v = attn_bwd(lengths, ohk, ohq, *tabs, csk, csq, okt, oqt, d_attn_b.reshape(2, QLEN, DIM), lse)

        d_bqkv = jnp.stack([jnp.sum(part, axis=(0, 1)) for part in (s_q, s_k, s_v)])
        s_all = jnp.concatenate([s_q, s_k, s_v, jnp.zeros((2, ROWS, 256), F32)], axis=2).reshape(2 * ROWS, 4 * QCOLS)
        s_mine = lax.dynamic_slice_in_dim(s_all, QCOLS * xi, QCOLS, axis=1)
        for hop in range(1, 4):
            part = lax.dynamic_slice_in_dim(s_all, QCOLS * ((xi + hop) % 4), QCOLS, axis=1)
            s_mine = s_mine + lax.ppermute(part, 'x', [(i, (i + hop) % 4) for i in range(4)])
        d_qkvw = lax.dot_general(h_rows.astype(F32), s_mine, (TN, ((), ())), precision=HIGH)
        d_h = lax.dot_general(s_mine, qkv_w.astype(F32), (NT, ((), ())), precision=HIGH)
        d_h = d_h.reshape(2, ROWS, DIM)[:, :VOCAB]
        d_e = ln_back(d_h, vecs[0], xhat1, inv1)
        d_e = d_e + jnp.einsum('bsv,bsd->bvd', oh_own, d_resid_b.reshape(2, QLEN, DIM), preferred_element_type=F32)
        d_table = jnp.sum(d_e * row_scale[:, :, None], axis=0)
        d_up_bias = jnp.sum(d_up_lin, axis=0).reshape(1, 2, DIM)
        d_up_bias = jnp.where(jnp.arange(2)[:, None, None] == ci, d_up_bias, 0.0).reshape(4, DIM)
        small = jnp.concatenate([
            d_table,
            jnp.sum(d_h * xhat1, axis=(0, 1))[None], jnp.sum(d_h, axis=(0, 1))[None], d_bqkv,
            jnp.sum(d_resid, axis=0)[None], jnp.sum(d_nm * xhat2, axis=0)[None], jnp.sum(d_nm, axis=0)[None],
            jnp.sum(grad32, axis=0)[None], d_up_bias, jnp.zeros((2, DIM), F32)], axis=0)
        r_out, r_qkv = reduce_oq(d_outw.reshape(16, 2, ROWS, DIM), d_qkvw.reshape(16, 2, ROWS, QCOLS))
        r_down = lax.psum_scatter(d_down, CHIP, scatter_dimension=0, tiled=True)
        r_up = lax.psum_scatter(d_up, CHIP, scatter_dimension=0, tiled=True)
        small, r_out = lax.optimization_barrier((small, r_out))
        r_up, r_down, small = reduce_last(r_up.reshape(2 * ROWS, 4, HALF_D).transpose(1, 0, 2), r_down.reshape(4, ROWS, DIM), small)
        r_up = r_up.transpose(1, 0, 2).reshape(2 * ROWS, FFH)
        r_down = r_down.reshape(160, DIM)
        small = small.transpose(1, 0, 2).reshape(SMALL, DIM)
        d_vecs = lax.dynamic_slice(small, (VOCAB, fi * ROWS), (9, ROWS))
        d_bup_half = lax.dynamic_slice_in_dim(small, VOCAB + 9 + 2 * ci, 2, axis=0).reshape(FFH)
        d_bup = lax.dynamic_slice_in_dim(d_bup_half, chip * 160, 160, axis=0)

        up_keep = lax.dynamic_slice_in_dim(r_up, ci * ROWS, ROWS, axis=0)
        up_give = lax.dynamic_slice_in_dim(r_up, (1 - ci) * ROWS, ROWS, axis=0)
        up_got = lax.ppermute(up_give, 'c', SWAP)
        r_up = jnp.stack([jnp.where(ci == 0, up_keep, up_got).reshape(ROWS, 16, 160),
                          jnp.where(ci == 0, up_got, up_keep).reshape(ROWS, 16, 160)], axis=2).reshape(ROWS, 5120)
        r_qkv = r_qkv[:, :3 * DIM].reshape(ROWS, 3, HEADS, HDIM)
        return layer_out, small[:VOCAB], d_vecs, r_qkv, r_out, r_up, d_bup, r_down

    in_specs = (P(FSDP, 'x'), P(FSDP), P(), P(None, FSDP), P(FSDP), P(FSDP), P(FSDP), P(FSDP), P(FSDP), P(FSDP, 'x'))
    out_specs = (P(FSDP, 'x'), P(), P(None, FSDP), P(FSDP), P(FSDP), P(FSDP), P(FSDP), P(FSDP))
    return jax.shard_map(local_step, mesh=mesh4, in_specs=in_specs, out_specs=out_specs, check_vma=False)
```

```python
import functools

import jax
import jax.numpy as jnp
from jax import lax
from jax.experimental import pallas as pl
from jax.experimental.pallas import tpu as pltpu
from jax.sharding import Mesh, PartitionSpec as P

MASK_ID = 32
VOCAB = 33
LN_EPS = 1e-5
ROPE_BASE = 10000.0
TRAIN_RATIO = 0.15 * 0.8
NEG_BIG = -1e30
SEQ = 1024
QLEN = 256
HEADS = 20
HDIM = 64
PAIRS = HEADS // 2
DIM = HEADS * HDIM
ROWS = 40
F32 = jnp.float32
BF16 = jnp.bfloat16
SWAP = [(0, 1), (1, 0)]
CHIP = ('z', 'y')
FSDP = ('z', 'y', 'c')
QCOLS = 1024
MESH = pl.DeviceIdType.MESH
LO, HI, ALL = range(3)
NT = ((1,), (1,))
TN = ((0,), (0,))
LANES = 128
HALF = HDIM // 2
FFH = 2 * DIM
TOK = 2 * QLEN
HALF_D = DIM // 2
COST = pl.CostEstimate(flops=20_000_000_000, bytes_accessed=15_000_000, transcendentals=10_000_000)
HIGH = lax.Precision.HIGHEST


def mm(a, b, dims=((1,), (0,))):
    return lax.dot_general(a, b, (dims, ((), ())), preferred_element_type=F32)


def ln_stats(z_in):
    row_mean = jnp.mean(z_in, axis=-1, keepdims=True)
    centered = z_in - row_mean
    row_var = jnp.mean(centered * centered, axis=-1, keepdims=True)
    inv = lax.rsqrt(row_var + LN_EPS)
    return centered * inv, inv


def ln_back(d_out, gain, xhat, inv):
    d_hat = d_out * gain
    m1 = jnp.mean(d_hat, axis=-1, keepdims=True)
    m2 = jnp.mean(d_hat * xhat, axis=-1, keepdims=True)
    return inv * (d_hat - m1 - xhat * m2)


def rot_half(z_in, sign):
    lane = lax.broadcasted_iota(jnp.int32, z_in.shape, 1)
    down, up = pltpu.roll(z_in, LANES - HALF, 1), pltpu.roll(z_in, HALF, 1)
    return jnp.where(lane % HDIM < HALF, -sign * down, sign * up)


def split3(z_in):
    hi = z_in.astype(BF16).astype(F32)
    rest = z_in - hi
    mid = rest.astype(BF16).astype(F32)
    return jnp.concatenate([hi, mid, rest - mid, jnp.zeros((LANES - 3 * ROWS, z_in.shape[1]), F32)], axis=0).astype(BF16)


def expand_qkv(ohk_ref, ohq_ref, tq_ref, tk_ref, tv_ref, csk_ref, csq_ref):
    ohk = ohk_ref[0]
    t_q = tq_ref[0] * HDIM ** -0.5
    z_q = mm(ohq_ref[0], split3(jnp.concatenate([t_q, rot_half(t_q, 1.0)], axis=1)))
    q = z_q[:, :LANES] * csq_ref[:, :LANES] + z_q[:, LANES:] * csq_ref[:, LANES:]
    t_k = tk_ref[0]
    z_k = mm(ohk, split3(jnp.concatenate([t_k, rot_half(t_k, 1.0)], axis=1)))
    k = z_k[:, :LANES] * csk_ref[:, :LANES] + z_k[:, LANES:] * csk_ref[:, LANES:]
    t_v = jnp.concatenate([tv_ref[0], jnp.zeros((LANES - ROWS, LANES), F32)], axis=0)
    v = mm(ohk, t_v.astype(BF16))
    return q, k.astype(BF16), v.astype(BF16)


def head_masks():
    low = lax.broadcasted_iota(jnp.int32, (QLEN, LANES), 1) < HDIM
    return low, jnp.logical_not(low)


def key_mask(seq_len):
    return lax.broadcasted_iota(jnp.int32, (SEQ, QLEN), 0) < seq_len


def head_cols(head):
    return slice(HDIM * head, HDIM * (head + 1))


def attn_fwd_kernel(len_ref, ohk_ref, ohq_ref, tq_ref, tk_ref, tv_ref, csk_ref, csq_ref, o_ref, lse_ref):
    q, k, v = expand_qkv(ohk_ref, ohq_ref, tq_ref, tk_ref, tv_ref, csk_ref, csq_ref)
    key_ok = lax.broadcasted_iota(jnp.int32, (QLEN, SEQ), 1) < len_ref[pl.program_id(0)]
    outs, stats = [], []
    for mine in head_masks():
        q_h = jnp.where(mine, q, 0.0).astype(BF16)
        s = jnp.where(key_ok, mm(q_h, k, NT), NEG_BIG)
        top = jnp.max(s, axis=-1, keepdims=True)
        e = jnp.exp(s - top)
        total = jnp.sum(e, axis=-1, keepdims=True)
        outs.append(mm(e.astype(BF16), v) / total)
        stats.append(jnp.broadcast_to(top + jnp.log(total), (QLEN, LANES)))
    low = head_masks()[0]
    o_ref[0] = jnp.where(low, *outs).astype(BF16)
    stats = jnp.where(low, *stats).T
    lse_ref[0, 0, :2, :] = jnp.concatenate([stats[:1], stats[HDIM:HDIM + 1]], axis=0)


def attn_bwd_kernel(len_ref, ohk_ref, ohq_ref, tq_ref, tk_ref, tv_ref, csk_ref, csq_ref, okt_ref, oqt_ref, do_ref, lse_ref, sq_ref, sk_ref, sv_ref):
    q, k, v = expand_qkv(ohk_ref, ohq_ref, tq_ref, tk_ref, tv_ref, csk_ref, csq_ref)
    d_o = do_ref[0]
    key_ok = key_mask(len_ref[pl.program_id(0)])
    k_t = k.T
    dv, dk, dqs = None, None, []
    for head, mine in enumerate(head_masks()):
        q_h = jnp.where(mine, q, 0.0).astype(BF16)
        do_h = jnp.where(mine, d_o, jnp.zeros_like(d_o))
        p = jnp.where(key_ok, jnp.exp(mm(k, q_h, NT) - lse_ref[0, 0, head:head + 1, :]), 0.0)
        t = p * mm(v, do_h, NT)
        ds = (t - p * jnp.sum(t, axis=0, keepdims=True)).astype(BF16)
        dv_h = mm(p.astype(BF16), do_h)
        dk_h = mm(ds, q_h)
        dv = dv_h if dv is None else dv + dv_h
        dk = dk_h if dk is None else dk + dk_h
        dqs.append(mm(k_t[head_cols(head)], ds))
    dq = jnp.concatenate(dqs, axis=0).T

    def by_token(onehot_t, d_in):
        return mm(onehot_t, d_in.astype(BF16))
    s_q = by_token(oqt_ref[0], jnp.concatenate([dq * csq_ref[:, :LANES], dq * csq_ref[:, LANES:]], axis=1))
    sq_ref[0] = (s_q[:, :LANES] + rot_half(s_q[:, LANES:], -1.0)) * HDIM ** -0.5
    s_k = by_token(okt_ref[0], jnp.concatenate([dk * csk_ref[:, :LANES], dk * csk_ref[:, LANES:]], axis=1))
    sk_ref[0] = s_k[:, :LANES] + rot_half(s_k[:, LANES:], -1.0)
    sv_ref[0] = by_token(okt_ref[0], dv)


def tab_spec():
    return pl.BlockSpec((1, ROWS, LANES), lambda b, j: (b, 0, j))


def attn_specs():
    return [
        pl.BlockSpec(memory_space=pltpu.SMEM),
        pl.BlockSpec((1, SEQ, LANES), lambda b, j: (b, 0, 0)),
        pl.BlockSpec((1, QLEN, LANES), lambda b, j: (b, 0, 0)),
        tab_spec(),
        tab_spec(),
        tab_spec(),
        pl.BlockSpec((SEQ, 256), lambda b, j: (0, 0)),
        pl.BlockSpec((QLEN, 256), lambda b, j: (0, 0)),
    ]


def row_spec():
    return pl.BlockSpec((1, QLEN, LANES), lambda b, j: (b, 0, j))


def lse_spec():
    return pl.BlockSpec((1, 1, 8, QLEN), lambda b, j: (b, j, 0, 0))


def attn_fwd(lengths, ohk, ohq, tq, tk, tv, csk, csq):
    return pl.pallas_call(
        attn_fwd_kernel, grid=(2, PAIRS), in_specs=attn_specs(), out_specs=[row_spec(), lse_spec()],
        out_shape=[jax.ShapeDtypeStruct((2, QLEN, DIM), BF16), jax.ShapeDtypeStruct((2, PAIRS, 8, QLEN), F32)],
        cost_estimate=COST,
        name='attn_fwd')(lengths, ohk, ohq, tq, tk, tv, csk, csq)


def attn_bwd(lengths, ohk, ohq, tq, tk, tv, csk, csq, okt, oqt, d_o, lse):
    return pl.pallas_call(
        attn_bwd_kernel, grid=(2, PAIRS), in_specs=attn_specs() + [pl.BlockSpec((1, ROWS, SEQ), lambda b, j: (b, 0, 0)), pl.BlockSpec((1, ROWS, QLEN), lambda b, j: (b, 0, 0)), row_spec(), lse_spec()],
        out_specs=[tab_spec()] * 3, out_shape=[jax.ShapeDtypeStruct((2, ROWS, DIM), F32)] * 3,
        cost_estimate=COST,
        name='attn_bwd')(lengths, ohk, ohq, tq, tk, tv, csk, csq, okt, oqt, d_o, lse)


class Ring:
    def __init__(self, axis, ports):
        self.me = lax.axis_index(axis)
        self.axis, self.ports = axis, ports
        self.right = lax.rem(self.me + 1, 4)
        self.left = lax.rem(self.me + 3, 4)
        self.far = lax.rem(self.me + 2, 4)
        self.open = []

    def send(self, src, dst, to):
        copy = remote(src, dst, next(self.ports), {self.axis: to})
        copy.start()
        self.open.append(copy)
        return copy

    def drain(self):
        for copy in self.open:
            copy.wait_send()
        self.open = []

    def rs_start(self, chunk, bufs):
        self.chunk = chunk
        self.b1, self.b2, self.b3, self.b4, self.b5, self.b6 = bufs
        self.m1 = self.send(chunk(self.far, LO), self.b1, self.right)
        self.m3 = self.send(chunk(self.far, HI), self.b3, self.left)
        self.m2 = self.send(chunk(self.right, HI), self.b2, self.right)
        self.m4 = self.send(chunk(self.left, LO), self.b4, self.left)

    def rs_mid(self):
        self.m1.wait_recv()
        self.b1[...] += self.chunk(self.right, LO)[...]
        self.m5 = self.send(self.b1, self.b5, self.right)
        self.m3.wait_recv()
        self.b3[...] += self.chunk(self.left, HI)[...]
        self.m6 = self.send(self.b3, self.b6, self.left)

    def rs_end(self):
        self.m4.wait_recv()
        self.m5.wait_recv()
        low = self.chunk(self.me, LO)[...] + self.b4[...] + self.b5[...]
        self.m2.wait_recv()
        self.m6.wait_recv()
        high = self.chunk(self.me, HI)[...] + self.b2[...] + self.b6[...]
        self.drain()
        return low, high

    def ag_start(self, slot, own=None, split=True):
        self.slot, self.split = slot, split
        home = slot(self.me, ALL)
        own = home if own is None else own
        self.a1 = self.send(own, home, self.right)
        self.a2 = self.send(own, home, self.left)

    def ag_mid(self):
        self.a1.wait_recv()
        part = self.slot(self.left, LO if self.split else ALL)
        self.a3 = self.send(part, part, self.right)
        self.a2.wait_recv()
        if self.split:
            part = self.slot(self.right, HI)
            self.a4 = self.send(part, part, self.left)

    def ag_end(self):
        self.a3.wait_recv()
        if self.split:
            self.a4.wait_recv()
        self.drain()


def meet():
    barrier = pltpu.get_barrier_semaphore()
    for axis in ('x', 'z', 'y'):
        me = lax.axis_index(axis)
        for step in (1, 3):
            pl.semaphore_signal(barrier, inc=1, device_id={axis: lax.rem(me + step, 4)}, device_id_type=MESH)
    pl.semaphore_signal(barrier, inc=1, device_id={'c': 1 - lax.axis_index('c')}, device_id_type=MESH)
    pl.semaphore_wait(barrier, 7)


def ports_of(sends, recvs):
    return ((sends.at[i], recvs.at[i]) for i in range(sends.shape[0]))


def remote(src, dst, port, target):
    return pltpu.make_async_remote_copy(src_ref=src, dst_ref=dst, send_sem=port[0], recv_sem=port[-1], device_id=target, device_id_type=MESH)


def core_copy(src, dst, ports):
    return remote(src, dst, next(ports), {'c': 1 - lax.axis_index('c')})


CUT = 24
UP_R = 80
HALF_W = 1152
WIDE = DIM + QCOLS


def half_rows(half):
    return pl.ds(0, CUT) if half == LO else pl.ds(CUT, ROWS - CUT)


def up_rows(half):
    return pl.ds(UP_R // 2 * half, UP_R // 2)


def ring_bufs(lead, width):
    return [pltpu.VMEM(lead + (CUT if i in (0, 3, 4) else ROWS - CUT, width), F32) for i in range(6)]


def oq_kernel(d_out_ref, d_qkv_ref, down_ref, out_ref, qkv_ref, down_out, acc, one_a, one_b, gath, *rest):
    bufs, ports = [rest[6 * i:6 * i + 6] for i in range(5)], ports_of(*rest[-2:])
    ci = lax.axis_index('c')
    meet()
    first = core_copy(d_out_ref.at[:, 1 - ci], acc.at[:, :, pl.ds(0, DIM)], ports)
    second = core_copy(d_qkv_ref.at[:, 1 - ci], acc.at[:, :, pl.ds(DIM, QCOLS)], ports)
    first.start()
    second.start()
    xd, gd = Ring('x', ports), Ring('x', ports)
    xd.rs_start(lambda k, h: down_ref.at[k, half_rows(h)], bufs[4])
    first.wait_recv()

    def add_out(i, carry):
        acc[i, :, :DIM] += d_out_ref[i, ci]
        return carry
    lax.fori_loop(0, 16, add_out, 0)
    second.wait_recv()

    def add_qkv(i, carry):
        acc[i, :, DIM:] += d_qkv_ref[i, ci]
        return carry
    lax.fori_loop(0, 16, add_qkv, 0)
    grid = acc.reshape(4, 4, ROWS, WIDE)
    ya = Ring('y', ports)
    zb = Ring('z', ports)
    ya.rs_start(lambda k, h: grid.at[:, k, half_rows(h), pl.ds(0, HALF_W)], bufs[0])
    zb.rs_start(lambda k, h: grid.at[k, :, half_rows(h), pl.ds(HALF_W, HALF_W)], bufs[1])
    xd.rs_mid()
    ya.rs_mid()
    zb.rs_mid()
    low, high = xd.rs_end()
    down_out[xd.me, half_rows(LO)] = low
    down_out[xd.me, half_rows(HI)] = high
    gd.ag_start(lambda k, h: down_out.at[k] if h == ALL else down_out.at[k, half_rows(h)])
    one_a[:, :CUT], one_a[:, CUT:] = ya.rs_end()
    za = Ring('z', ports)
    za.rs_start(lambda k, h: one_a.at[k, half_rows(h)], bufs[2])
    one_b[:, :CUT], one_b[:, CUT:] = zb.rs_end()
    yb = Ring('y', ports)
    yb.rs_start(lambda k, h: one_b.at[k, half_rows(h)], bufs[3])
    za.rs_mid()
    yb.rs_mid()
    gd.ag_mid()
    gd.ag_end()
    xr = Ring('x', ports)
    low, high = za.rs_end()
    gath[xr.me, :CUT, :HALF_W] = low
    gath[xr.me, CUT:, :HALF_W] = high
    low, high = yb.rs_end()
    gath[xr.me, :CUT, HALF_W:] = low
    gath[xr.me, CUT:, HALF_W:] = high
    xr.ag_start(lambda k, h: gath.at[k] if h == ALL else gath.at[k, half_rows(h)])
    xr.ag_mid()
    xr.ag_end()
    out_ref[...] = (gath[0, :, :DIM] + gath[1, :, :DIM]) + (gath[2, :, :DIM] + gath[3, :, :DIM])
    for k in range(4):
        qkv_ref[:, QCOLS * k:QCOLS * (k + 1)] = gath[k, :, DIM:]
    first.wait_send()
    second.wait_send()


def vmem(n):
    return [pl.BlockSpec(memory_space=pltpu.VMEM)] * n


def reduce_oq(d_out, d_qkv, down):
    return pl.pallas_call(
        oq_kernel, in_specs=vmem(3), out_specs=vmem(3),
        out_shape=[jax.ShapeDtypeStruct((ROWS, DIM), F32), jax.ShapeDtypeStruct((ROWS, 4 * QCOLS), F32), jax.ShapeDtypeStruct((4, ROWS, DIM), F32)],
        scratch_shapes=[pltpu.VMEM((16, ROWS, WIDE), F32), pltpu.VMEM((4, ROWS, HALF_W), F32), pltpu.VMEM((4, ROWS, HALF_W), F32),
                        pltpu.VMEM((4, ROWS, WIDE), F32)]
        + ring_bufs((4,), HALF_W) + ring_bufs((4,), HALF_W) + ring_bufs((), HALF_W) + ring_bufs((), HALF_W) + ring_bufs((), DIM)
        + [pltpu.SemaphoreType.DMA((40,)), pltpu.SemaphoreType.DMA((40,))],
        compiler_params=pltpu.CompilerParams(collective_id=1, has_side_effects=True, vmem_limit_bytes=56 * 1024 * 1024),
        cost_estimate=COST,
        name='reduce_oq')(d_out, d_qkv, down)


def first_kernel(wq_ref, wo_ref, pack_ref, tok_ref, gq, go, gp, gt, sends, recvs):
    ports = ports_of(sends, recvs)
    ci = lax.axis_index('c')
    y1, z1, yp, xt = Ring('y', ports), Ring('z', ports), Ring('y', ports), Ring('x', ports)
    y2, z2, zp = Ring('y', ports), Ring('z', ports), Ring('z', ports)
    yi, zi = y1.me, z1.me
    meet()
    y1.ag_start(lambda k, h: gq.at[zi, k, ci] if h == ALL else gq.at[zi, k, ci, :, pl.ds(QCOLS // 2 * h, QCOLS // 2)], wq_ref)
    z1.ag_start(lambda k, h: go.at[k, yi, ci] if h == ALL else go.at[k, yi, ci, :, pl.ds(HALF_D * h, HALF_D)], wo_ref)
    yp.ag_start(lambda k, h: gp.at[zi, k, ci], pack_ref, False)
    xt.ag_start(lambda k, h: gt.at[k], tok_ref, False)
    gq[zi, yi, ci] = wq_ref[...]
    go[zi, yi, ci] = wo_ref[...]
    gp[zi, yi, ci] = pack_ref[...]
    gt[xt.me] = tok_ref[...]
    stage = (y1, z1, yp, xt)
    for ring in stage:
        ring.ag_mid()
    for ring in stage:
        ring.ag_end()
    z2.ag_start(lambda k, h: gq.at[k, :, ci] if h == ALL else gq.at[k, pl.ds(2 * h, 2), ci])
    y2.ag_start(lambda k, h: go.at[:, k, ci] if h == ALL else go.at[pl.ds(2 * h, 2), k, ci])
    zp.ag_start(lambda k, h: gp.at[k, :, ci], None, False)
    stage = (z2, y2, zp)
    for ring in stage:
        ring.ag_mid()
    for ring in stage:
        ring.ag_end()
    swaps = [core_copy(ref.at[:, :, ci], ref.at[:, :, ci], ports) for ref in (gq, go, gp)]
    for swap in swaps:
        swap.start()
    for swap in swaps:
        swap.wait_recv()
        swap.wait_send()


def gather_first(wq, wo, pack, tok):
    return pl.pallas_call(
        first_kernel, in_specs=vmem(4), out_specs=vmem(4),
        out_shape=[jax.ShapeDtypeStruct((4, 4, 2) + wq.shape, BF16), jax.ShapeDtypeStruct((4, 4, 2) + wo.shape, BF16),
                   jax.ShapeDtypeStruct((4, 4, 2) + pack.shape, F32), jax.ShapeDtypeStruct((4,) + tok.shape, jnp.int32)],
        scratch_shapes=[pltpu.SemaphoreType.DMA((28,)), pltpu.SemaphoreType.DMA((28,))],
        compiler_params=pltpu.CompilerParams(collective_id=3, has_side_effects=True, vmem_limit_bytes=24 * 1024 * 1024),
        cost_estimate=COST, name='gather_first')(wq, wo, pack, tok)


SMALL = 48


def last_kernel(up_ref, small_ref, up_out, small_out, pair, sum_y, sum_z, sum_x, *rest):
    bufs, ports = rest[:6], ports_of(*rest[-2:])
    ci = lax.axis_index('c')
    meet()
    swap = core_copy(small_ref, pair, ports)
    swap.start()
    xu = Ring('x', ports)
    xu.rs_start(lambda k, h: up_ref.at[k, up_rows(h)], bufs)
    swap.wait_recv()
    both = small_ref[...] + pair[...]
    mine = jnp.where(ci == 0, both[:, 0:HALF_D], both[:, HALF_D:1280])

    def gather(ref):
        return lambda k, h: ref.at[k] if h == ALL else ref.at[k, pl.ds(24 * h, 24)]

    def total(ref):
        return (ref[0] + ref[1]) + (ref[2] + ref[3])
    ys = Ring('y', ports)
    sum_y[ys.me] = mine
    ys.ag_start(gather(sum_y))
    xu.rs_mid()
    ys.ag_mid()
    ys.ag_end()
    zs = Ring('z', ports)
    sum_z[zs.me] = total(sum_y)
    zs.ag_start(gather(sum_z))
    low, high = xu.rs_end()
    up_out[xu.me, up_rows(LO)] = low
    up_out[xu.me, up_rows(HI)] = high
    gu = Ring('x', ports)
    gu.ag_start(lambda k, h: up_out.at[k] if h == ALL else up_out.at[k, up_rows(h)])
    zs.ag_mid()
    zs.ag_end()
    xs = Ring('x', ports)
    sum_x[xs.me] = total(sum_z)
    xs.ag_start(gather(sum_x))
    gu.ag_mid()
    xs.ag_mid()
    xs.ag_end()
    small_out[ci] = total(sum_x)
    back = core_copy(small_out.at[ci], small_out.at[ci], ports)
    back.start()
    gu.ag_end()
    back.wait_recv()
    back.wait_send()
    swap.wait_send()


def reduce_last(up, small):
    up_bufs = [pltpu.VMEM((UP_R // 2, HALF_D), F32) for _ in range(6)]
    return pl.pallas_call(
        last_kernel, in_specs=vmem(2), out_specs=vmem(2),
        out_shape=[jax.ShapeDtypeStruct((4, UP_R, HALF_D), F32), jax.ShapeDtypeStruct((2, SMALL, HALF_D), F32)],
        scratch_shapes=[pltpu.VMEM((SMALL, DIM), F32)] + [pltpu.VMEM((4, SMALL, HALF_D), F32)] * 3 + up_bufs
        + [pltpu.SemaphoreType.DMA((34,)), pltpu.SemaphoreType.DMA((34,))],
        compiler_params=pltpu.CompilerParams(collective_id=2, has_side_effects=True, vmem_limit_bytes=40 * 1024 * 1024),
        name='reduce_last')(up, small)


def one_hot3(tok):
    lanes = jnp.arange(LANES)
    return ((tok[..., None] == lanes % ROWS) & (lanes < 3 * ROWS)).astype(BF16)


def solution(mesh):
    mesh4 = Mesh(mesh.devices.reshape(4, 4, 4, 2), ('x', 'z', 'y', 'c'))

    def local_step(tokens, lengths, embed_table, layer_vecs, w_qkv, w_out, w_up, b_up, w_down, grad_out):
        xi = lax.axis_index('x')
        ci = lax.axis_index('c')
        chip = lax.axis_index('z') * 4 + lax.axis_index('y')
        fi = chip * 2 + ci
        wq_loc = lax.dynamic_slice_in_dim(jnp.pad(w_qkv.reshape(ROWS, 3 * DIM), ((0, 0), (0, 256))), QCOLS * xi, QCOLS, axis=1)
        packed = jnp.concatenate([layer_vecs.reshape(360), b_up, jnp.zeros((504,), F32)]).reshape(8, LANES)
        up_loc = w_up.reshape(ROWS, 16, 2, 160)
        up_mine = lax.dynamic_index_in_dim(up_loc, ci, axis=2, keepdims=False).reshape(ROWS, FFH)
        up_send = lax.dynamic_index_in_dim(up_loc, 1 - ci, axis=2, keepdims=False).reshape(ROWS, FFH)
        up_recv = lax.ppermute(up_send, 'c', SWAP)
        up_pair = jnp.concatenate([jnp.where(ci == 0, up_mine, up_recv), jnp.where(ci == 0, up_recv, up_mine)], axis=0)
        up_pair, packed = lax.optimization_barrier((up_pair, packed))
        up_w = lax.all_gather(up_pair, CHIP, axis=0, tiled=True)
        down_w = lax.all_gather(w_down, CHIP, axis=0, tiled=True)
        qkv_w, out_w, packed, tok_all = gather_first(wq_loc, w_out, packed, tokens.reshape(4, LANES))
        qkv_w, out_w, packed = qkv_w.reshape(DIM, QCOLS), out_w.reshape(DIM, DIM), packed.reshape(32, 8 * LANES)
        tok_all = tok_all.reshape(4, 2, QLEN).transpose(1, 0, 2).reshape(2, SEQ)
        vecs = packed[:, :360].reshape(32, 9, ROWS).transpose(1, 0, 2).reshape(9, DIM)
        up_b = lax.dynamic_index_in_dim(packed[:, 360:520].reshape(16, 2, 160), ci, axis=1, keepdims=False).reshape(FFH)
        grad_own = grad_out.reshape(TOK, DIM)
        grad2 = jnp.concatenate([grad_own, lax.ppermute(grad_own, 'c', SWAP)], axis=0)

        positions = jnp.arange(SEQ)
        tok_eff = jnp.where(positions[None, :] < lengths[:, None], tok_all, MASK_ID)
        tok_own = lax.dynamic_slice_in_dim(tok_eff, xi * QLEN, QLEN, axis=1)
        mask_count = jnp.sum((tok_all == MASK_ID).astype(F32), axis=1)
        drop_scale = (1.0 - TRAIN_RATIO) / (1.0 - mask_count / lengths.astype(F32))
        ohk = one_hot3(tok_eff)
        ohq = one_hot3(tok_own)
        oh_own = ohq[:, :, :VOCAB]
        rows = jnp.arange(ROWS)[:, None]
        okt = (tok_eff[:, None, :] == rows).astype(BF16)
        oqt = (tok_own[:, None, :] == rows).astype(BF16)
        row_scale = jnp.where(jnp.arange(VOCAB)[None, :] == MASK_ID, 0.0, drop_scale[:, None])
        e_rows = embed_table.astype(F32)[None] * row_scale[:, :, None]
        xhat1, inv1 = ln_stats(e_rows)
        h_rows = (xhat1 * vecs[0] + vecs[1]).astype(BF16)
        h_rows = jnp.pad(h_rows, ((0, 0), (0, ROWS - VOCAB), (0, 0))).reshape(2 * ROWS, DIM)
        t_loc = mm(h_rows, qkv_w)
        t_all = jnp.zeros((2 * ROWS, 4 * QCOLS), F32)
        for hop in range(4):
            part = lax.ppermute(t_loc, 'x', [(i, (i + hop) % 4) for i in range(4)]) if hop else t_loc
            t_all = lax.dynamic_update_slice_in_dim(t_all, part, QCOLS * ((xi + 4 - hop) % 4), axis=1)
        t_all = (t_all[:, :3 * DIM] + vecs[2:5].reshape(1, 3 * DIM)).reshape(2, ROWS, 3 * DIM)
        tabs = (t_all[:, :, :DIM], t_all[:, :, DIM:2 * DIM], t_all[:, :, 2 * DIM:])
        inv_freq = 1.0 / (ROPE_BASE ** (jnp.arange(0, HDIM, 2, dtype=F32) / HDIM))
        angles = positions.astype(F32)[:, None] * inv_freq[None, :]
        csk = jnp.concatenate([jnp.tile(jnp.cos(angles), (1, 4)), jnp.tile(jnp.sin(angles), (1, 4))], axis=1)
        csq = lax.dynamic_slice_in_dim(csk, xi * QLEN, QLEN, axis=0)

        attn_o, lse = attn_fwd(lengths, ohk, ohq, *tabs, csk, csq)
        attn_o2 = attn_o.reshape(TOK, DIM)
        keep_own = jnp.where(tok_own == MASK_ID, 0.0, drop_scale[:, None])
        embedded = jnp.einsum('bsv,vd->bsd', oh_own, embed_table, preferred_element_type=F32) * keep_own[:, :, None]
        x1 = embedded.reshape(TOK, DIM) + mm(attn_o2, out_w) + vecs[5]
        xhat2, inv2 = ln_stats(x1)
        nm = (xhat2 * vecs[6] + vecs[7]).astype(BF16)
        nm2 = jnp.concatenate([nm, lax.ppermute(nm, 'c', SWAP)], axis=0)
        nm2, up_w = lax.optimization_barrier((nm2, up_w))
        up_lin = mm(nm2, up_w) + up_b
        cdf = 0.5 * (1.0 + lax.erf(up_lin * 0.7071067811865476))
        gelu_b = (up_lin * cdf).astype(BF16)
        slope = cdf + up_lin * (0.3989422804014327 * jnp.exp(-0.5 * up_lin * up_lin))
        down2 = mm(gelu_b, down_w)
        down_got = lax.ppermute(down2[TOK:], 'c', SWAP)
        layer_out = (x1 + down2[:TOK] + down_got + vecs[8]).astype(BF16).reshape(2, QLEN, DIM)

        d_down = mm(gelu_b, grad2, TN)
        d_down, grad2 = lax.optimization_barrier((d_down, grad2))
        d_up_lin = mm(grad2, down_w, NT) * slope
        d_up_b = d_up_lin.astype(BF16)
        d_up = mm(nm2, d_up_b, TN)
        d_nm2 = mm(d_up_b, up_w, NT)
        d_nm = d_nm2[:TOK] + lax.ppermute(d_nm2[TOK:], 'c', SWAP)
        grad32 = grad_own.astype(F32)
        d_resid = grad32 + ln_back(d_nm, vecs[6], xhat2, inv2)
        d_resid_b = d_resid.astype(BF16)
        d_outw = mm(attn_o2, d_resid_b, TN)
        d_attn_b = mm(d_resid_b, out_w, NT).astype(BF16)
        s_q, s_k, s_v = attn_bwd(lengths, ohk, ohq, *tabs, csk, csq, okt, oqt, d_attn_b.reshape(2, QLEN, DIM), lse)

        d_bqkv = jnp.stack([jnp.sum(part, axis=(0, 1)) for part in (s_q, s_k, s_v)])
        s_all = jnp.concatenate([s_q, s_k, s_v, jnp.zeros((2, ROWS, 256), F32)], axis=2).reshape(2 * ROWS, 4 * QCOLS)
        s_mine = lax.dynamic_slice_in_dim(s_all, QCOLS * xi, QCOLS, axis=1)
        for hop in range(1, 4):
            part = lax.dynamic_slice_in_dim(s_all, QCOLS * ((xi + hop) % 4), QCOLS, axis=1)
            s_mine = s_mine + lax.ppermute(part, 'x', [(i, (i + hop) % 4) for i in range(4)])
        d_qkvw = lax.dot_general(h_rows.astype(F32), s_mine, (TN, ((), ())), precision=HIGH)
        d_h = lax.dot_general(s_mine, qkv_w.astype(F32), (NT, ((), ())), precision=HIGH)
        d_h = d_h.reshape(2, ROWS, DIM)[:, :VOCAB]
        d_e = ln_back(d_h, vecs[0], xhat1, inv1)
        d_e = d_e + jnp.einsum('bsv,bsd->bvd', oh_own, d_resid_b.reshape(2, QLEN, DIM), preferred_element_type=F32)
        d_table = jnp.sum(d_e * row_scale[:, :, None], axis=0)
        d_up_bias = jnp.sum(d_up_lin, axis=0).reshape(1, 2, DIM)
        d_up_bias = jnp.where(jnp.arange(2)[:, None, None] == ci, d_up_bias, 0.0).reshape(4, DIM)
        small = jnp.concatenate([
            d_table,
            jnp.sum(d_h * xhat1, axis=(0, 1))[None], jnp.sum(d_h, axis=(0, 1))[None], d_bqkv,
            jnp.sum(d_resid, axis=0)[None], jnp.sum(d_nm * xhat2, axis=0)[None], jnp.sum(d_nm, axis=0)[None],
            jnp.sum(grad32, axis=0)[None], d_up_bias, jnp.zeros((2, DIM), F32)], axis=0)
        r_down = lax.psum_scatter(d_down, CHIP, scatter_dimension=0, tiled=True)
        r_up = lax.psum_scatter(d_up, CHIP, scatter_dimension=0, tiled=True)
        r_up = r_up.reshape(UP_R, 4, HALF_D).transpose(1, 0, 2)
        r_out, r_qkv, r_down = reduce_oq(d_outw.reshape(16, 2, ROWS, DIM), d_qkvw.reshape(16, 2, ROWS, QCOLS), r_down.reshape(4, ROWS, DIM))
        small, r_out = lax.optimization_barrier((small, r_out))
        r_up, small = reduce_last(r_up, small)
        r_up = r_up.transpose(1, 0, 2).reshape(2 * ROWS, FFH)
        r_down = r_down.reshape(160, DIM)
        small = small.transpose(1, 0, 2).reshape(SMALL, DIM)
        d_vecs = lax.dynamic_slice(small, (VOCAB, fi * ROWS), (9, ROWS))
        d_bup_half = lax.dynamic_slice_in_dim(small, VOCAB + 9 + 2 * ci, 2, axis=0).reshape(FFH)
        d_bup = lax.dynamic_slice_in_dim(d_bup_half, chip * 160, 160, axis=0)

        up_keep = lax.dynamic_slice_in_dim(r_up, ci * ROWS, ROWS, axis=0)
        up_give = lax.dynamic_slice_in_dim(r_up, (1 - ci) * ROWS, ROWS, axis=0)
        up_got = lax.ppermute(up_give, 'c', SWAP)
        r_up = jnp.stack([jnp.where(ci == 0, up_keep, up_got).reshape(ROWS, 16, 160),
                          jnp.where(ci == 0, up_got, up_keep).reshape(ROWS, 16, 160)], axis=2).reshape(ROWS, 5120)
        r_qkv = r_qkv[:, :3 * DIM].reshape(ROWS, 3, HEADS, HDIM)
        return layer_out, small[:VOCAB], d_vecs, r_qkv, r_out, r_up, d_bup, r_down

    in_specs = (P(FSDP, 'x'), P(FSDP), P(), P(None, FSDP), P(FSDP), P(FSDP), P(FSDP), P(FSDP), P(FSDP), P(FSDP, 'x'))
    out_specs = (P(FSDP, 'x'), P(), P(None, FSDP), P(FSDP), P(FSDP), P(FSDP), P(FSDP), P(FSDP))
    return jax.shard_map(local_step, mesh=mesh4, in_specs=in_specs, out_specs=out_specs, check_vma=False)
```

```python
import functools

import jax
import jax.numpy as jnp
from jax import lax
from jax.experimental import pallas as pl
from jax.experimental.pallas import tpu as pltpu
from jax.sharding import Mesh, PartitionSpec as P

MASK_ID = 32
VOCAB = 33
LN_EPS = 1e-5
ROPE_BASE = 10000.0
TRAIN_RATIO = 0.15 * 0.8
NEG_BIG = -1e30
SEQ = 1024
QLEN = 256
HEADS = 20
HDIM = 64
PAIRS = HEADS // 2
DIM = HEADS * HDIM
ROWS = 40
F32 = jnp.float32
BF16 = jnp.bfloat16
SWAP = [(0, 1), (1, 0)]
CHIP = ('z', 'y')
FSDP = ('z', 'y', 'c')
QCOLS = 1024
MESH = pl.DeviceIdType.MESH
LO, HI, ALL = range(3)
NT = ((1,), (1,))
TN = ((0,), (0,))
LANES = 128
HALF = HDIM // 2
FFH = 2 * DIM
TOK = 2 * QLEN
HALF_D = DIM // 2
COST = pl.CostEstimate(flops=20_000_000_000, bytes_accessed=15_000_000, transcendentals=10_000_000)
HIGH = lax.Precision.HIGHEST


def mm(a, b, dims=((1,), (0,))):
    return lax.dot_general(a, b, (dims, ((), ())), preferred_element_type=F32)


def ln_stats(z_in):
    row_mean = jnp.mean(z_in, axis=-1, keepdims=True)
    centered = z_in - row_mean
    row_var = jnp.mean(centered * centered, axis=-1, keepdims=True)
    inv = lax.rsqrt(row_var + LN_EPS)
    return centered * inv, inv


def ln_back(d_out, gain, xhat, inv):
    d_hat = d_out * gain
    m1 = jnp.mean(d_hat, axis=-1, keepdims=True)
    m2 = jnp.mean(d_hat * xhat, axis=-1, keepdims=True)
    return inv * (d_hat - m1 - xhat * m2)


def rot_half(z_in, sign):
    lane = lax.broadcasted_iota(jnp.int32, z_in.shape, 1)
    down, up = pltpu.roll(z_in, LANES - HALF, 1), pltpu.roll(z_in, HALF, 1)
    return jnp.where(lane % HDIM < HALF, -sign * down, sign * up)


def split3(z_in):
    hi = z_in.astype(BF16).astype(F32)
    rest = z_in - hi
    mid = rest.astype(BF16).astype(F32)
    return jnp.concatenate([hi, mid, rest - mid, jnp.zeros((LANES - 3 * ROWS, z_in.shape[1]), F32)], axis=0).astype(BF16)


def expand_qkv(ohk_ref, ohq_ref, tq_ref, tk_ref, tv_ref, csk_ref, csq_ref):
    ohk = ohk_ref[0]
    t_q = tq_ref[0] * HDIM ** -0.5
    z_q = mm(ohq_ref[0], split3(jnp.concatenate([t_q, rot_half(t_q, 1.0)], axis=1)))
    q = z_q[:, :LANES] * csq_ref[:, :LANES] + z_q[:, LANES:] * csq_ref[:, LANES:]
    t_k = tk_ref[0]
    z_k = mm(ohk, split3(jnp.concatenate([t_k, rot_half(t_k, 1.0)], axis=1)))
    k = z_k[:, :LANES] * csk_ref[:, :LANES] + z_k[:, LANES:] * csk_ref[:, LANES:]
    t_v = jnp.concatenate([tv_ref[0], jnp.zeros((LANES - ROWS, LANES), F32)], axis=0)
    v = mm(ohk, t_v.astype(BF16))
    return q, k.astype(BF16), v.astype(BF16)


def head_masks():
    low = lax.broadcasted_iota(jnp.int32, (QLEN, LANES), 1) < HDIM
    return low, jnp.logical_not(low)


def key_mask(seq_len):
    return lax.broadcasted_iota(jnp.int32, (SEQ, QLEN), 0) < seq_len


def head_cols(head):
    return slice(HDIM * head, HDIM * (head + 1))


def attn_fwd_kernel(len_ref, ohk_ref, ohq_ref, tq_ref, tk_ref, tv_ref, csk_ref, csq_ref, o_ref, lse_ref):
    q, k, v = expand_qkv(ohk_ref, ohq_ref, tq_ref, tk_ref, tv_ref, csk_ref, csq_ref)
    key_ok = lax.broadcasted_iota(jnp.int32, (QLEN, SEQ), 1) < len_ref[pl.program_id(0)]
    outs, stats = [], []
    for mine in head_masks():
        q_h = jnp.where(mine, q, 0.0).astype(BF16)
        s = jnp.where(key_ok, mm(q_h, k, NT), NEG_BIG)
        top = jnp.max(s, axis=-1, keepdims=True)
        e = jnp.exp(s - top)
        total = jnp.sum(e, axis=-1, keepdims=True)
        outs.append(mm(e.astype(BF16), v) / total)
        stats.append(jnp.broadcast_to(top + jnp.log(total), (QLEN, LANES)))
    low = head_masks()[0]
    o_ref[0] = jnp.where(low, *outs).astype(BF16)
    stats = jnp.where(low, *stats).T
    lse_ref[0, 0, :2, :] = jnp.concatenate([stats[:1], stats[HDIM:HDIM + 1]], axis=0)


def attn_bwd_kernel(len_ref, ohk_ref, ohq_ref, tq_ref, tk_ref, tv_ref, csk_ref, csq_ref, okt_ref, oqt_ref, do_ref, lse_ref, sq_ref, sk_ref, sv_ref):
    q, k, v = expand_qkv(ohk_ref, ohq_ref, tq_ref, tk_ref, tv_ref, csk_ref, csq_ref)
    d_o = do_ref[0]
    key_ok = key_mask(len_ref[pl.program_id(0)])
    k_t = k.T
    dv, dk, dqs = None, None, []
    for head, mine in enumerate(head_masks()):
        q_h = jnp.where(mine, q, 0.0).astype(BF16)
        do_h = jnp.where(mine, d_o, jnp.zeros_like(d_o))
        p = jnp.where(key_ok, jnp.exp(mm(k, q_h, NT) - lse_ref[0, 0, head:head + 1, :]), 0.0)
        t = p * mm(v, do_h, NT)
        ds = (t - p * jnp.sum(t, axis=0, keepdims=True)).astype(BF16)
        dv_h = mm(p.astype(BF16), do_h)
        dk_h = mm(ds, q_h)
        dv = dv_h if dv is None else dv + dv_h
        dk = dk_h if dk is None else dk + dk_h
        dqs.append(mm(k_t[head_cols(head)], ds))
    dq = jnp.concatenate(dqs, axis=0).T

    def by_token(onehot_t, d_in):
        return mm(onehot_t, d_in.astype(BF16))
    s_q = by_token(oqt_ref[0], jnp.concatenate([dq * csq_ref[:, :LANES], dq * csq_ref[:, LANES:]], axis=1))
    sq_ref[0] = (s_q[:, :LANES] + rot_half(s_q[:, LANES:], -1.0)) * HDIM ** -0.5
    s_k = by_token(okt_ref[0], jnp.concatenate([dk * csk_ref[:, :LANES], dk * csk_ref[:, LANES:]], axis=1))
    sk_ref[0] = s_k[:, :LANES] + rot_half(s_k[:, LANES:], -1.0)
    sv_ref[0] = by_token(okt_ref[0], dv)


def tab_spec():
    return pl.BlockSpec((1, ROWS, LANES), lambda b, j: (b, 0, j))


def attn_specs():
    return [
        pl.BlockSpec(memory_space=pltpu.SMEM),
        pl.BlockSpec((1, SEQ, LANES), lambda b, j: (b, 0, 0)),
        pl.BlockSpec((1, QLEN, LANES), lambda b, j: (b, 0, 0)),
        tab_spec(),
        tab_spec(),
        tab_spec(),
        pl.BlockSpec((SEQ, 256), lambda b, j: (0, 0)),
        pl.BlockSpec((QLEN, 256), lambda b, j: (0, 0)),
    ]


def row_spec():
    return pl.BlockSpec((1, QLEN, LANES), lambda b, j: (b, 0, j))


def lse_spec():
    return pl.BlockSpec((1, 1, 8, QLEN), lambda b, j: (b, j, 0, 0))


def attn_fwd(lengths, ohk, ohq, tq, tk, tv, csk, csq):
    return pl.pallas_call(
        attn_fwd_kernel, grid=(2, PAIRS), in_specs=attn_specs(), out_specs=[row_spec(), lse_spec()],
        out_shape=[jax.ShapeDtypeStruct((2, QLEN, DIM), BF16), jax.ShapeDtypeStruct((2, PAIRS, 8, QLEN), F32)],
        cost_estimate=COST,
        name='attn_fwd')(lengths, ohk, ohq, tq, tk, tv, csk, csq)


def attn_bwd(lengths, ohk, ohq, tq, tk, tv, csk, csq, okt, oqt, d_o, lse):
    return pl.pallas_call(
        attn_bwd_kernel, grid=(2, PAIRS), in_specs=attn_specs() + [pl.BlockSpec((1, ROWS, SEQ), lambda b, j: (b, 0, 0)), pl.BlockSpec((1, ROWS, QLEN), lambda b, j: (b, 0, 0)), row_spec(), lse_spec()],
        out_specs=[tab_spec()] * 3, out_shape=[jax.ShapeDtypeStruct((2, ROWS, DIM), F32)] * 3,
        cost_estimate=COST,
        name='attn_bwd')(lengths, ohk, ohq, tq, tk, tv, csk, csq, okt, oqt, d_o, lse)


class Ring:
    def __init__(self, axis, ports):
        self.me = lax.axis_index(axis)
        self.axis, self.ports = axis, ports
        self.right = lax.rem(self.me + 1, 4)
        self.left = lax.rem(self.me + 3, 4)
        self.far = lax.rem(self.me + 2, 4)
        self.open = []

    def send(self, src, dst, to):
        copy = remote(src, dst, next(self.ports), {self.axis: to})
        copy.start()
        self.open.append(copy)
        return copy

    def drain(self):
        for copy in self.open:
            copy.wait_send()
        self.open = []

    def rs_start(self, chunk, bufs):
        self.chunk = chunk
        self.b1, self.b2, self.b3, self.b4, self.b5, self.b6 = bufs
        self.m1 = self.send(chunk(self.far, LO), self.b1, self.right)
        self.m3 = self.send(chunk(self.far, HI), self.b3, self.left)
        self.m2 = self.send(chunk(self.right, HI), self.b2, self.right)
        self.m4 = self.send(chunk(self.left, LO), self.b4, self.left)

    def rs_mid(self):
        self.m1.wait_recv()
        self.b1[...] += self.chunk(self.right, LO)[...]
        self.m5 = self.send(self.b1, self.b5, self.right)
        self.m3.wait_recv()
        self.b3[...] += self.chunk(self.left, HI)[...]
        self.m6 = self.send(self.b3, self.b6, self.left)

    def rs_end(self):
        self.m4.wait_recv()
        self.m5.wait_recv()
        low = self.chunk(self.me, LO)[...] + self.b4[...] + self.b5[...]
        self.m2.wait_recv()
        self.m6.wait_recv()
        high = self.chunk(self.me, HI)[...] + self.b2[...] + self.b6[...]
        self.drain()
        return low, high

    def ag_start(self, slot, own=None, split=True):
        self.slot, self.split = slot, split
        home = slot(self.me, ALL)
        own = home if own is None else own
        self.a1 = self.send(own, home, self.right)
        self.a2 = self.send(own, home, self.left)

    def ag_mid(self):
        self.a1.wait_recv()
        part = self.slot(self.left, LO if self.split else ALL)
        self.a3 = self.send(part, part, self.right)
        self.a2.wait_recv()
        if self.split:
            part = self.slot(self.right, HI)
            self.a4 = self.send(part, part, self.left)

    def ag_end(self):
        self.a3.wait_recv()
        if self.split:
            self.a4.wait_recv()
        self.drain()


def meet():
    barrier = pltpu.get_barrier_semaphore()
    for axis in ('x', 'z', 'y'):
        me = lax.axis_index(axis)
        for step in (1, 3):
            pl.semaphore_signal(barrier, inc=1, device_id={axis: lax.rem(me + step, 4)}, device_id_type=MESH)
    pl.semaphore_signal(barrier, inc=1, device_id={'c': 1 - lax.axis_index('c')}, device_id_type=MESH)
    pl.semaphore_wait(barrier, 7)


def ports_of(sends, recvs):
    return ((sends.at[i], recvs.at[i]) for i in range(sends.shape[0]))


def remote(src, dst, port, target):
    return pltpu.make_async_remote_copy(src_ref=src, dst_ref=dst, send_sem=port[0], recv_sem=port[-1], device_id=target, device_id_type=MESH)


def core_copy(src, dst, ports):
    return remote(src, dst, next(ports), {'c': 1 - lax.axis_index('c')})


CUT = 24
UP_R = 80
HALF_W = 1152
WIDE = DIM + QCOLS


def half_rows(half):
    return pl.ds(0, CUT) if half == LO else pl.ds(CUT, ROWS - CUT)


def up_rows(half):
    return pl.ds(UP_R // 2 * half, UP_R // 2)


def ring_bufs(lead, width):
    return [pltpu.VMEM(lead + (CUT if i in (0, 3, 4) else ROWS - CUT, width), F32) for i in range(6)]


def oq_kernel(d_out_ref, d_qkv_ref, down_ref, out_ref, qkv_ref, down_out, acc, one_a, one_b, gath, *rest):
    bufs, ports = [rest[6 * i:6 * i + 6] for i in range(5)], ports_of(*rest[-2:])
    ci = lax.axis_index('c')
    meet()
    first = core_copy(d_out_ref.at[:, 1 - ci], acc.at[:, :, pl.ds(0, DIM)], ports)
    second = core_copy(d_qkv_ref.at[:, 1 - ci], acc.at[:, :, pl.ds(DIM, QCOLS)], ports)
    first.start()
    second.start()
    xd, gd = Ring('x', ports), Ring('x', ports)
    xd.rs_start(lambda k, h: down_ref.at[k, half_rows(h)], bufs[4])
    first.wait_recv()

    def add_out(i, carry):
        acc[i, :, :DIM] += d_out_ref[i, ci]
        return carry
    lax.fori_loop(0, 16, add_out, 0)
    grid = acc.reshape(4, 4, ROWS, WIDE)
    ya = Ring('y', ports)
    ya.rs_start(lambda k, h: grid.at[:, k, half_rows(h), pl.ds(0, HALF_W)], bufs[0])
    second.wait_recv()

    def add_qkv(i, carry):
        acc[i, :, DIM:] += d_qkv_ref[i, ci]
        return carry
    lax.fori_loop(0, 16, add_qkv, 0)
    zb = Ring('z', ports)
    zb.rs_start(lambda k, h: grid.at[k, :, half_rows(h), pl.ds(HALF_W, HALF_W)], bufs[1])
    xd.rs_mid()
    ya.rs_mid()
    zb.rs_mid()
    low, high = xd.rs_end()
    down_out[xd.me, half_rows(LO)] = low
    down_out[xd.me, half_rows(HI)] = high
    gd.ag_start(lambda k, h: down_out.at[k] if h == ALL else down_out.at[k, half_rows(h)])
    one_a[:, :CUT], one_a[:, CUT:] = ya.rs_end()
    za = Ring('z', ports)
    za.rs_start(lambda k, h: one_a.at[k, half_rows(h)], bufs[2])
    one_b[:, :CUT], one_b[:, CUT:] = zb.rs_end()
    yb = Ring('y', ports)
    yb.rs_start(lambda k, h: one_b.at[k, half_rows(h)], bufs[3])
    za.rs_mid()
    yb.rs_mid()
    gd.ag_mid()
    gd.ag_end()
    xr = Ring('x', ports)
    low, high = za.rs_end()
    gath[xr.me, :CUT, :HALF_W] = low
    gath[xr.me, CUT:, :HALF_W] = high
    low, high = yb.rs_end()
    gath[xr.me, :CUT, HALF_W:] = low
    gath[xr.me, CUT:, HALF_W:] = high
    xr.ag_start(lambda k, h: gath.at[k] if h == ALL else gath.at[k, half_rows(h)])
    xr.ag_mid()
    xr.ag_end()
    out_ref[...] = (gath[0, :, :DIM] + gath[1, :, :DIM]) + (gath[2, :, :DIM] + gath[3, :, :DIM])
    for k in range(4):
        qkv_ref[:, QCOLS * k:QCOLS * (k + 1)] = gath[k, :, DIM:]
    first.wait_send()
    second.wait_send()


def vmem(n):
    return [pl.BlockSpec(memory_space=pltpu.VMEM)] * n


def reduce_oq(d_out, d_qkv, down):
    return pl.pallas_call(
        oq_kernel, in_specs=vmem(3), out_specs=vmem(3),
        out_shape=[jax.ShapeDtypeStruct((ROWS, DIM), F32), jax.ShapeDtypeStruct((ROWS, 4 * QCOLS), F32), jax.ShapeDtypeStruct((4, ROWS, DIM), F32)],
        scratch_shapes=[pltpu.VMEM((16, ROWS, WIDE), F32), pltpu.VMEM((4, ROWS, HALF_W), F32), pltpu.VMEM((4, ROWS, HALF_W), F32),
                        pltpu.VMEM((4, ROWS, WIDE), F32)]
        + ring_bufs((4,), HALF_W) + ring_bufs((4,), HALF_W) + ring_bufs((), HALF_W) + ring_bufs((), HALF_W) + ring_bufs((), DIM)
        + [pltpu.SemaphoreType.DMA((40,)), pltpu.SemaphoreType.DMA((40,))],
        compiler_params=pltpu.CompilerParams(collective_id=1, has_side_effects=True, vmem_limit_bytes=56 * 1024 * 1024),
        cost_estimate=COST,
        name='reduce_oq')(d_out, d_qkv, down)


def first_kernel(wq_ref, wo_ref, pack_ref, tok_ref, gq, go, gp, gt, sends, recvs):
    ports = ports_of(sends, recvs)
    ci = lax.axis_index('c')
    y1, z1, yp, xt = Ring('y', ports), Ring('z', ports), Ring('y', ports), Ring('x', ports)
    y2, z2, zp = Ring('y', ports), Ring('z', ports), Ring('z', ports)
    yi, zi = y1.me, z1.me
    meet()
    y1.ag_start(lambda k, h: gq.at[zi, k, ci] if h == ALL else gq.at[zi, k, ci, :, pl.ds(QCOLS // 2 * h, QCOLS // 2)], wq_ref)
    z1.ag_start(lambda k, h: go.at[k, yi, ci] if h == ALL else go.at[k, yi, ci, :, pl.ds(HALF_D * h, HALF_D)], wo_ref)
    yp.ag_start(lambda k, h: gp.at[zi, k, ci], pack_ref, False)
    xt.ag_start(lambda k, h: gt.at[k], tok_ref, False)
    gq[zi, yi, ci] = wq_ref[...]
    go[zi, yi, ci] = wo_ref[...]
    gp[zi, yi, ci] = pack_ref[...]
    gt[xt.me] = tok_ref[...]
    stage = (y1, z1, yp, xt)
    for ring in stage:
        ring.ag_mid()
    for ring in stage:
        ring.ag_end()
    z2.ag_start(lambda k, h: gq.at[k, :, ci] if h == ALL else gq.at[k, pl.ds(2 * h, 2), ci])
    y2.ag_start(lambda k, h: go.at[:, k, ci] if h == ALL else go.at[pl.ds(2 * h, 2), k, ci])
    zp.ag_start(lambda k, h: gp.at[k, :, ci], None, False)
    stage = (z2, y2, zp)
    for ring in stage:
        ring.ag_mid()
    for ring in stage:
        ring.ag_end()
    swaps = [core_copy(ref.at[:, :, ci], ref.at[:, :, ci], ports) for ref in (gq, go, gp)]
    for swap in swaps:
        swap.start()
    for swap in swaps:
        swap.wait_recv()
        swap.wait_send()


def gather_first(wq, wo, pack, tok):
    return pl.pallas_call(
        first_kernel, in_specs=vmem(4), out_specs=vmem(4),
        out_shape=[jax.ShapeDtypeStruct((4, 4, 2) + wq.shape, BF16), jax.ShapeDtypeStruct((4, 4, 2) + wo.shape, BF16),
                   jax.ShapeDtypeStruct((4, 4, 2) + pack.shape, F32), jax.ShapeDtypeStruct((4,) + tok.shape, jnp.int32)],
        scratch_shapes=[pltpu.SemaphoreType.DMA((28,)), pltpu.SemaphoreType.DMA((28,))],
        compiler_params=pltpu.CompilerParams(collective_id=3, has_side_effects=True, vmem_limit_bytes=24 * 1024 * 1024),
        cost_estimate=COST, name='gather_first')(wq, wo, pack, tok)


SMALL = 48


def last_kernel(up_ref, small_ref, up_out, small_out, pair, sum_y, sum_z, sum_x, *rest):
    bufs, ports = rest[:6], ports_of(*rest[-2:])
    ci = lax.axis_index('c')
    meet()
    swap = core_copy(small_ref, pair, ports)
    swap.start()
    xu = Ring('x', ports)
    xu.rs_start(lambda k, h: up_ref.at[k, up_rows(h)], bufs)
    swap.wait_recv()
    both = small_ref[...] + pair[...]
    mine = jnp.where(ci == 0, both[:, 0:HALF_D], both[:, HALF_D:1280])

    def gather(ref):
        return lambda k, h: ref.at[k] if h == ALL else ref.at[k, pl.ds(24 * h, 24)]

    def total(ref):
        return (ref[0] + ref[1]) + (ref[2] + ref[3])
    ys = Ring('y', ports)
    sum_y[ys.me] = mine
    ys.ag_start(gather(sum_y))
    xu.rs_mid()
    ys.ag_mid()
    ys.ag_end()
    zs = Ring('z', ports)
    sum_z[zs.me] = total(sum_y)
    zs.ag_start(gather(sum_z))
    low, high = xu.rs_end()
    up_out[xu.me, up_rows(LO)] = low
    up_out[xu.me, up_rows(HI)] = high
    gu = Ring('x', ports)
    gu.ag_start(lambda k, h: up_out.at[k] if h == ALL else up_out.at[k, up_rows(h)])
    zs.ag_mid()
    zs.ag_end()
    xs = Ring('x', ports)
    sum_x[xs.me] = total(sum_z)
    xs.ag_start(gather(sum_x))
    gu.ag_mid()
    xs.ag_mid()
    xs.ag_end()
    small_out[ci] = total(sum_x)
    back = core_copy(small_out.at[ci], small_out.at[ci], ports)
    back.start()
    gu.ag_end()
    back.wait_recv()
    back.wait_send()
    swap.wait_send()


def reduce_last(up, small):
    up_bufs = [pltpu.VMEM((UP_R // 2, HALF_D), F32) for _ in range(6)]
    return pl.pallas_call(
        last_kernel, in_specs=vmem(2), out_specs=vmem(2),
        out_shape=[jax.ShapeDtypeStruct((4, UP_R, HALF_D), F32), jax.ShapeDtypeStruct((2, SMALL, HALF_D), F32)],
        scratch_shapes=[pltpu.VMEM((SMALL, DIM), F32)] + [pltpu.VMEM((4, SMALL, HALF_D), F32)] * 3 + up_bufs
        + [pltpu.SemaphoreType.DMA((34,)), pltpu.SemaphoreType.DMA((34,))],
        compiler_params=pltpu.CompilerParams(collective_id=2, has_side_effects=True, vmem_limit_bytes=40 * 1024 * 1024),
        name='reduce_last')(up, small)


def one_hot3(tok):
    lanes = jnp.arange(LANES)
    return ((tok[..., None] == lanes % ROWS) & (lanes < 3 * ROWS)).astype(BF16)


def solution(mesh):
    mesh4 = Mesh(mesh.devices.reshape(4, 4, 4, 2), ('x', 'z', 'y', 'c'))

    def local_step(tokens, lengths, embed_table, layer_vecs, w_qkv, w_out, w_up, b_up, w_down, grad_out):
        xi = lax.axis_index('x')
        ci = lax.axis_index('c')
        chip = lax.axis_index('z') * 4 + lax.axis_index('y')
        fi = chip * 2 + ci
        wq_loc = lax.dynamic_slice_in_dim(jnp.pad(w_qkv.reshape(ROWS, 3 * DIM), ((0, 0), (0, 256))), QCOLS * xi, QCOLS, axis=1)
        packed = jnp.concatenate([layer_vecs.reshape(360), b_up, jnp.zeros((504,), F32)]).reshape(8, LANES)
        up_loc = w_up.reshape(ROWS, 16, 2, 160)
        up_mine = lax.dynamic_index_in_dim(up_loc, ci, axis=2, keepdims=False).reshape(ROWS, FFH)
        up_send = lax.dynamic_index_in_dim(up_loc, 1 - ci, axis=2, keepdims=False).reshape(ROWS, FFH)
        up_recv = lax.ppermute(up_send, 'c', SWAP)
        up_pair = jnp.concatenate([jnp.where(ci == 0, up_mine, up_recv), jnp.where(ci == 0, up_recv, up_mine)], axis=0)
        up_pair, packed = lax.optimization_barrier((up_pair, packed))
        up_w = lax.all_gather(up_pair, CHIP, axis=0, tiled=True)
        down_w = lax.all_gather(w_down, CHIP, axis=0, tiled=True)
        qkv_w, out_w, packed, tok_all = gather_first(wq_loc, w_out, packed, tokens.reshape(4, LANES))
        qkv_w, out_w, packed = qkv_w.reshape(DIM, QCOLS), out_w.reshape(DIM, DIM), packed.reshape(32, 8 * LANES)
        tok_all = tok_all.reshape(4, 2, QLEN).transpose(1, 0, 2).reshape(2, SEQ)
        vecs = packed[:, :360].reshape(32, 9, ROWS).transpose(1, 0, 2).reshape(9, DIM)
        up_b = lax.dynamic_index_in_dim(packed[:, 360:520].reshape(16, 2, 160), ci, axis=1, keepdims=False).reshape(FFH)
        grad_own = grad_out.reshape(TOK, DIM)
        grad2 = jnp.concatenate([grad_own, lax.ppermute(grad_own, 'c', SWAP)], axis=0)

        positions = jnp.arange(SEQ)
        tok_eff = jnp.where(positions[None, :] < lengths[:, None], tok_all, MASK_ID)
        tok_own = lax.dynamic_slice_in_dim(tok_eff, xi * QLEN, QLEN, axis=1)
        mask_count = jnp.sum((tok_all == MASK_ID).astype(F32), axis=1)
        drop_scale = (1.0 - TRAIN_RATIO) / (1.0 - mask_count / lengths.astype(F32))
        ohk = one_hot3(tok_eff)
        ohq = one_hot3(tok_own)
        oh_own = ohq[:, :, :VOCAB]
        rows = jnp.arange(ROWS)[:, None]
        okt = (tok_eff[:, None, :] == rows).astype(BF16)
        oqt = (tok_own[:, None, :] == rows).astype(BF16)
        row_scale = jnp.where(jnp.arange(VOCAB)[None, :] == MASK_ID, 0.0, drop_scale[:, None])
        e_rows = embed_table.astype(F32)[None] * row_scale[:, :, None]
        xhat1, inv1 = ln_stats(e_rows)
        h_rows = (xhat1 * vecs[0] + vecs[1]).astype(BF16)
        h_rows = jnp.pad(h_rows, ((0, 0), (0, ROWS - VOCAB), (0, 0))).reshape(2 * ROWS, DIM)
        t_loc = mm(h_rows, qkv_w)
        t_all = jnp.zeros((2 * ROWS, 4 * QCOLS), F32)
        for hop in range(4):
            part = lax.ppermute(t_loc, 'x', [(i, (i + hop) % 4) for i in range(4)]) if hop else t_loc
            t_all = lax.dynamic_update_slice_in_dim(t_all, part, QCOLS * ((xi + 4 - hop) % 4), axis=1)
        t_all = (t_all[:, :3 * DIM] + vecs[2:5].reshape(1, 3 * DIM)).reshape(2, ROWS, 3 * DIM)
        tabs = (t_all[:, :, :DIM], t_all[:, :, DIM:2 * DIM], t_all[:, :, 2 * DIM:])
        inv_freq = 1.0 / (ROPE_BASE ** (jnp.arange(0, HDIM, 2, dtype=F32) / HDIM))
        angles = positions.astype(F32)[:, None] * inv_freq[None, :]
        csk = jnp.concatenate([jnp.tile(jnp.cos(angles), (1, 4)), jnp.tile(jnp.sin(angles), (1, 4))], axis=1)
        csq = lax.dynamic_slice_in_dim(csk, xi * QLEN, QLEN, axis=0)

        attn_o, lse = attn_fwd(lengths, ohk, ohq, *tabs, csk, csq)
        attn_o2 = attn_o.reshape(TOK, DIM)
        keep_own = jnp.where(tok_own == MASK_ID, 0.0, drop_scale[:, None])
        embedded = jnp.einsum('bsv,vd->bsd', oh_own, embed_table, preferred_element_type=F32) * keep_own[:, :, None]
        x1 = embedded.reshape(TOK, DIM) + mm(attn_o2, out_w) + vecs[5]
        xhat2, inv2 = ln_stats(x1)
        nm = (xhat2 * vecs[6] + vecs[7]).astype(BF16)
        nm2 = jnp.concatenate([nm, lax.ppermute(nm, 'c', SWAP)], axis=0)
        nm2, up_w = lax.optimization_barrier((nm2, up_w))
        up_lin = mm(nm2, up_w) + up_b
        cdf = 0.5 * (1.0 + lax.erf(up_lin * 0.7071067811865476))
        gelu_b = (up_lin * cdf).astype(BF16)
        slope = cdf + up_lin * (0.3989422804014327 * jnp.exp(-0.5 * up_lin * up_lin))
        down2 = mm(gelu_b, down_w)
        down_got = lax.ppermute(down2[TOK:], 'c', SWAP)
        layer_out = (x1 + down2[:TOK] + down_got + vecs[8]).astype(BF16).reshape(2, QLEN, DIM)

        d_down = mm(gelu_b, grad2, TN)
        d_down, grad2 = lax.optimization_barrier((d_down, grad2))
        d_up_lin = mm(grad2, down_w, NT) * slope
        d_up_b = d_up_lin.astype(BF16)
        d_up = mm(nm2, d_up_b, TN)
        d_nm2 = mm(d_up_b, up_w, NT)
        d_nm = d_nm2[:TOK] + lax.ppermute(d_nm2[TOK:], 'c', SWAP)
        grad32 = grad_own.astype(F32)
        d_resid = grad32 + ln_back(d_nm, vecs[6], xhat2, inv2)
        d_resid_b = d_resid.astype(BF16)
        d_outw = mm(attn_o2, d_resid_b, TN)
        d_attn_b = mm(d_resid_b, out_w, NT).astype(BF16)
        s_q, s_k, s_v = attn_bwd(lengths, ohk, ohq, *tabs, csk, csq, okt, oqt, d_attn_b.reshape(2, QLEN, DIM), lse)

        d_bqkv = jnp.stack([jnp.sum(part, axis=(0, 1)) for part in (s_q, s_k, s_v)])
        s_all = jnp.concatenate([s_q, s_k, s_v, jnp.zeros((2, ROWS, 256), F32)], axis=2).reshape(2 * ROWS, 4 * QCOLS)
        s_mine = lax.dynamic_slice_in_dim(s_all, QCOLS * xi, QCOLS, axis=1)
        for hop in range(1, 4):
            part = lax.dynamic_slice_in_dim(s_all, QCOLS * ((xi + hop) % 4), QCOLS, axis=1)
            s_mine = s_mine + lax.ppermute(part, 'x', [(i, (i + hop) % 4) for i in range(4)])
        d_qkvw = lax.dot_general(h_rows.astype(F32), s_mine, (TN, ((), ())), precision=HIGH)
        d_h = lax.dot_general(s_mine, qkv_w.astype(F32), (NT, ((), ())), precision=HIGH)
        d_h = d_h.reshape(2, ROWS, DIM)[:, :VOCAB]
        d_e = ln_back(d_h, vecs[0], xhat1, inv1)
        d_e = d_e + jnp.einsum('bsv,bsd->bvd', oh_own, d_resid_b.reshape(2, QLEN, DIM), preferred_element_type=F32)
        d_table = jnp.sum(d_e * row_scale[:, :, None], axis=0)
        d_up_bias = jnp.sum(d_up_lin, axis=0).reshape(1, 2, DIM)
        d_up_bias = jnp.where(jnp.arange(2)[:, None, None] == ci, d_up_bias, 0.0).reshape(4, DIM)
        small = jnp.concatenate([
            d_table,
            jnp.sum(d_h * xhat1, axis=(0, 1))[None], jnp.sum(d_h, axis=(0, 1))[None], d_bqkv,
            jnp.sum(d_resid, axis=0)[None], jnp.sum(d_nm * xhat2, axis=0)[None], jnp.sum(d_nm, axis=0)[None],
            jnp.sum(grad32, axis=0)[None], d_up_bias, jnp.zeros((2, DIM), F32)], axis=0)
        r_down = lax.psum_scatter(d_down, CHIP, scatter_dimension=0, tiled=True)
        r_up = lax.psum_scatter(d_up, CHIP, scatter_dimension=0, tiled=True)
        r_up = r_up.reshape(UP_R, 4, HALF_D).transpose(1, 0, 2)
        r_out, r_qkv, r_down = reduce_oq(d_outw.reshape(16, 2, ROWS, DIM), d_qkvw.reshape(16, 2, ROWS, QCOLS), r_down.reshape(4, ROWS, DIM))
        small, r_out = lax.optimization_barrier((small, r_out))
        r_up, small = reduce_last(r_up, small)
        r_up = r_up.transpose(1, 0, 2).reshape(2 * ROWS, FFH)
        r_down = r_down.reshape(160, DIM)
        small = small.transpose(1, 0, 2).reshape(SMALL, DIM)
        d_vecs = lax.dynamic_slice(small, (VOCAB, fi * ROWS), (9, ROWS))
        d_bup_half = lax.dynamic_slice_in_dim(small, VOCAB + 9 + 2 * ci, 2, axis=0).reshape(FFH)
        d_bup = lax.dynamic_slice_in_dim(d_bup_half, chip * 160, 160, axis=0)

        up_keep = lax.dynamic_slice_in_dim(r_up, ci * ROWS, ROWS, axis=0)
        up_give = lax.dynamic_slice_in_dim(r_up, (1 - ci) * ROWS, ROWS, axis=0)
        up_got = lax.ppermute(up_give, 'c', SWAP)
        r_up = jnp.stack([jnp.where(ci == 0, up_keep, up_got).reshape(ROWS, 16, 160),
                          jnp.where(ci == 0, up_got, up_keep).reshape(ROWS, 16, 160)], axis=2).reshape(ROWS, 5120)
        r_qkv = r_qkv[:, :3 * DIM].reshape(ROWS, 3, HEADS, HDIM)
        return layer_out, small[:VOCAB], d_vecs, r_qkv, r_out, r_up, d_bup, r_down

    in_specs = (P(FSDP, 'x'), P(FSDP), P(), P(None, FSDP), P(FSDP), P(FSDP), P(FSDP), P(FSDP), P(FSDP), P(FSDP, 'x'))
    out_specs = (P(FSDP, 'x'), P(), P(None, FSDP), P(FSDP), P(FSDP), P(FSDP), P(FSDP), P(FSDP))
    return jax.shard_map(local_step, mesh=mesh4, in_specs=in_specs, out_specs=out_specs, check_vma=False)
```
